32 devices in a mesh: fsdp: 8 (over y, x, core), rep: 4 (over z).
Axes of the slice: x: 2, y: 2, z: 4, core: 2. Of those that a mesh axis runs over, the one named last changes fastest.
Arguments:
- hidden_in: bfloat16 [64, 512, 768], P(('fsdp', 'rep')), may hold values from -6 to 6
- lengths: int32 [64], P(('fsdp', 'rep')), may hold values from 128 to 512, as said below
- query_weight: bfloat16 [768, 768], P(('fsdp', 'rep')), may hold values from -0.21875 to 0.21875
- key_weight: bfloat16 [768, 768], P(('fsdp', 'rep')), may hold values from -0.21875 to 0.21875
- value_weight: bfloat16 [768, 768], P(('fsdp', 'rep')), may hold values from -0.21875 to 0.21875
- out_weight: bfloat16 [768, 768], P(('fsdp', 'rep')), may hold values from -3 to 3
- up_weight: bfloat16 [768, 3072], P(('fsdp', 'rep')), may hold values from -0.21875 to 0.21875
- down_weight: bfloat16 [3072, 768], P(('fsdp', 'rep')), may hold values from -0.109375 to 0.109375
- query_bias: bfloat16 [768], P(('fsdp', 'rep')), may hold values from -1.796875 to 1.796875
- value_bias: bfloat16 [768], P(('fsdp', 'rep')), may hold values from -1.796875 to 1.796875
- out_bias: bfloat16 [768], P(('fsdp', 'rep')), may hold values from -1.796875 to 1.796875
- up_bias: bfloat16 [3072], P(('fsdp', 'rep')), may hold values from -1.796875 to 1.796875
- down_bias: bfloat16 [768], P(('fsdp', 'rep')), may hold values from -1.796875 to 1.796875
- first_gain: bfloat16 [768], P(('fsdp', 'rep')), may hold values from 0.5 to 1.5
- first_shift: bfloat16 [768], P(('fsdp', 'rep')), may hold values from -1.796875 to 1.796875
- second_gain: bfloat16 [768], P(('fsdp', 'rep')), may hold values from 0.5 to 1.5
- second_shift: bfloat16 [768], P(('fsdp', 'rep')), may hold values from -1.796875 to 1.796875
- cotangent: bfloat16 [64, 512, 768], P(('fsdp', 'rep')), may hold values from -6 to 6
Outputs:
- hidden_out: bfloat16 [64, 512, 768], P(('fsdp', 'rep'))
- input_grad: bfloat16 [64, 512, 768], P(('fsdp', 'rep'))
- query_weight_grad: float32 [768, 768], P(('fsdp', 'rep'))
- key_weight_grad: float32 [768, 768], P(('fsdp', 'rep'))
- value_weight_grad: float32 [768, 768], P(('fsdp', 'rep'))
- out_weight_grad: float32 [768, 768], P(('fsdp', 'rep'))
- up_weight_grad: float32 [768, 3072], P(('fsdp', 'rep'))
- down_weight_grad: float32 [3072, 768], P(('fsdp', 'rep'))
- query_bias_grad: float32 [768], P(('fsdp', 'rep'))
- value_bias_grad: float32 [768], P(('fsdp', 'rep'))
- out_bias_grad: float32 [768], P(('fsdp', 'rep'))
- up_bias_grad: float32 [3072], P(('fsdp', 'rep'))
- down_bias_grad: float32 [768], P(('fsdp', 'rep'))
- first_gain_grad: float32 [768], P(('fsdp', 'rep'))
- first_shift_grad: float32 [768], P(('fsdp', 'rep'))
- second_gain_grad: float32 [768], P(('fsdp', 'rep'))
- second_shift_grad: float32 [768], P(('fsdp', 'rep'))
The draws below stay inside these ranges and needn't reach their ends.
Inputs may be any that keep to these rules, and one draw needn't show every extreme that they name: `lengths`: one sequence fills all 512 slots and one has the fewest valid tokens.
All inputs are finite; a program needn't handle non-finite values.
Results may differ from the reference program's by a relative error of at most 0.015.
Values may be sent and summed in bfloat16 or wider, within the bound.
A program may use at most 192 MiB of HBM per device.

```python
import math
import jax
import jax.numpy as jnp
from jax import lax

D = 768
H = 12
HD = 64
FF = 3072
L = 512
SEQS = 64


def draw_lengths(key, part):
    spans = jax.random.randint(key, (SEQS,), L // 4, L + 1, dtype=jnp.int32)
    spans = spans.at[0].set(L)
    return spans.at[1].set(L // 4)


def strengthened(array, rng, source, target, shards_of, factor):
    def block_of(position):
        return (jnp.arange(array.shape[position]) // (array.shape[position] // shards_of)).reshape((-1,) + (1,) * (array.ndim - 1 - position))

    near = jax.random.permutation(rng, shards_of)[block_of(target)]
    far = (block_of(target) + shards_of // 2) % shards_of
    return jnp.where((block_of(source) == near) | (block_of(source) == far), factor * array, array)


def block_scale(own_key, dims, shards, least, top_value):
    loudness = 1.0
    for dim, shards_of in shards:
        steps = jax.random.uniform(jax.random.fold_in(jax.random.fold_in(own_key, 6), dim), (shards_of,), jnp.float32, least / len(shards), top_value / len(shards))
        loudness = loudness * jnp.repeat(jnp.exp(steps), dims[dim] // shards_of).reshape((-1,) + (1,) * (len(dims) - 1 - dim))
    return loudness


def scatter_about(rng, dims, width, bound, pieces=(), kind=jnp.bfloat16):
    result = jax.random.normal(rng, dims, jnp.float32) * width
    if len(pieces) > 0:
        result = block_scale(rng, dims, pieces, -0.22, 0.18) * result
    return jnp.clip(result, min=-bound, max=bound).astype(kind)


def noise_with(stream_key, shape, width, reach, shards, heavy, kind=jnp.bfloat16):
    drawn = width * jax.random.normal(stream_key, shape, jnp.float32)
    if shards:
        drawn = drawn * block_scale(stream_key, shape, shards, -0.22, 0.18)
    return jnp.clip(strengthened(drawn, jax.random.fold_in(stream_key, 3), *heavy), -reach, reach).astype(kind)


def setup_inputs(seed: int = 0) -> dict:
    arg_keys = jax.random.split(jax.random.key(seed), 19)
    hidden_in = scatter_about(arg_keys[0], (SEQS, L, D), 1.0, 6.0, ((0, 32),))
    lengths = draw_lengths(jax.random.fold_in(arg_keys[18], 71), 0)
    query_weight = scatter_about(arg_keys[2], (D, D), D ** -0.5, 0.21875, ((0, 32),))
    key_weight = scatter_about(arg_keys[3], (D, D), D ** -0.5, 0.21875, ((0, 32),))
    value_weight = scatter_about(arg_keys[4], (D, D), D ** -0.5, 0.21875, ((0, 32),))
    out_weight = scatter_about(arg_keys[5], (D, D), (max(D // 192, 1)) ** -0.5, 3.0, ((0, 32),))
    up_weight = scatter_about(arg_keys[6], (D, FF), D ** -0.5, 0.21875, ((0, 32),))
    down_weight = scatter_about(arg_keys[7], (FF, D), FF ** -0.5, 0.109375, ((0, 32),))
    query_bias = scatter_about(arg_keys[8], (D,), 0.3, 1.796875, ((0, 32),))
    value_bias = scatter_about(arg_keys[9], (D,), 0.3, 1.796875, ((0, 32),))
    out_bias = scatter_about(arg_keys[10], (D,), 0.3, 1.796875, ((0, 32),))
    up_bias = scatter_about(arg_keys[11], (FF,), 0.3, 1.796875, ((0, 32),))
    down_bias = scatter_about(arg_keys[12], (D,), 0.3, 1.796875, ((0, 32),))
    first_gain = jnp.clip(1.0 + 0.1 * jax.random.normal(arg_keys[13], (D,), jnp.float32), 0.5, 1.5).astype(jnp.bfloat16)
    first_shift = scatter_about(arg_keys[14], (D,), 0.3, 1.796875, ((0, 32),))
    second_gain = jnp.clip(1.0 + 0.1 * jax.random.normal(arg_keys[15], (D,), jnp.float32), 0.5, 1.5).astype(jnp.bfloat16)
    second_shift = scatter_about(arg_keys[16], (D,), 0.3, 1.796875, ((0, 32),))
    cotangent = noise_with(arg_keys[17], (SEQS, L, D), 1.0, 6.0, ((0, 32),), (0, 2, 32, 2.75))
    return dict(hidden_in=hidden_in, lengths=lengths, query_weight=query_weight, key_weight=key_weight, value_weight=value_weight, out_weight=out_weight, up_weight=up_weight, down_weight=down_weight, query_bias=query_bias, value_bias=value_bias, out_bias=out_bias, up_bias=up_bias, down_bias=down_bias, first_gain=first_gain, first_shift=first_shift, second_gain=second_gain, second_shift=second_shift, cotangent=cotangent)


@jax.custom_vjp
def low(v):
    return lax.optimization_barrier(v.astype(jnp.bfloat16)).astype(jnp.float32)

@jax.custom_vjp
def low_back(v):
    return v

def low_keep(v):
    return (low(v), None)

def low_pass(kept, grad):
    return (grad,)

def back_keep(v):
    return (v, None)

def back_low(kept, grad):
    return (low(grad),)
low.defvjp(low_keep, low_pass)
low_back.defvjp(back_keep, back_low)
EPS = 1e-06
HIGH = lax.Precision.HIGHEST

def project(left, weight):
    return jnp.einsum('bld,de->ble', left, weight, precision=HIGH)

def norm_rows(hidden, gain, shift):
    mean = lax.optimization_barrier(jnp.mean(hidden, axis=-1, keepdims=True))
    centred = hidden - mean
    variance = lax.optimization_barrier(jnp.mean(centred * centred, axis=-1, keepdims=True))
    return centred * lax.rsqrt(variance + EPS) * gain + shift

def layer(inputs, keep, weights):
    wq, wk, wv, wo, wi, wd, bq, bv, bo, bi, bd, g1, s1, g2, s2 = weights
    batch = inputs.shape[0]
    scale = 1.0 / math.sqrt(HD)
    query = low(low_back(project(inputs, wq) + bq)).reshape(batch, L, H, HD)
    keys = low(low_back(project(inputs, wk))).reshape(batch, L, H, HD)
    values = low(low_back(project(inputs, wv) + bv)).reshape(batch, L, H, HD)
    raw = jnp.einsum('bqhe,bkhe->bhqk', query, keys, precision=HIGH) * scale
    scores = jnp.where(keep[:, None, None, :], low_back(raw), -1e+30)
    probs = low(jax.nn.softmax(scores, axis=-1))
    context = jnp.einsum('bhqk,bkhe->bqhe', probs, values, precision=HIGH).reshape(batch, L, D)
    context = low(low_back(context))
    attn = low_back(project(context, wo) + bo)
    first = norm_rows(inputs + attn, g1, s1)
    inner = low_back(project(low(first), wi) + bi)
    active = low(jax.nn.gelu(inner, approximate=False))
    branch = low_back(project(active, wd) + bd)
    return norm_rows(first + branch, g2, s2)

def reference(hidden_in, lengths, query_weight, key_weight, value_weight, out_weight, up_weight, down_weight, query_bias, value_bias, out_bias, up_bias, down_bias, first_gain, first_shift, second_gain, second_shift, cotangent):
    weights = tuple((w.astype(jnp.float32) for w in (query_weight, key_weight, value_weight, out_weight, up_weight, down_weight, query_bias, value_bias, out_bias, up_bias, down_bias, first_gain, first_shift, second_gain, second_shift)))
    group = 4
    blocks = SEQS // group
    inputs = hidden_in.astype(jnp.float32).reshape(blocks, group, L, D)
    grads_in = cotangent.astype(jnp.float32).reshape(blocks, group, L, D)
    spans = lengths.reshape(blocks, group)
    zeros = tuple((jnp.zeros_like(w) for w in weights))

    def step(carry, block):
        x_block, g_block, span = block
        keep = jnp.arange(L, dtype=jnp.int32)[None, :] < span[:, None]
        out, pull = jax.vjp(lambda xx, ww: layer(xx, keep, ww), x_block, weights)
        grad_x, grad_w = pull(g_block)
        summed = tuple((c + g for c, g in zip(carry, grad_w)))
        return (summed, (out.astype(jnp.bfloat16), grad_x.astype(jnp.bfloat16)))
    total, (outs, grad_xs) = lax.scan(step, zeros, (inputs, grads_in, spans))
    return (outs.reshape(SEQS, L, D), grad_xs.reshape(SEQS, L, D), total[0], total[1], total[2], total[3], total[4], total[5], total[6], total[7], total[8], total[9], total[10], total[11], total[12], total[13], total[14])
```

```python
import functools
import math

import jax
import jax.numpy as jnp
from jax import lax
from jax.experimental import pallas as pl
from jax.experimental.pallas import tpu as pltpu
from jax.sharding import PartitionSpec as P

HD = 64
PAIR = 2 * HD
BF = jnp.bfloat16
F32 = jnp.float32


def nt(left, right):
    return lax.dot_general(left, right, (((1,), (1,)), ((), ())), preferred_element_type=F32)


def nn(left, right):
    return jnp.dot(left, right, preferred_element_type=F32)


def tn(left, right):
    return lax.dot_general(left, right, (((0,), (0,)), ((), ())), preferred_element_type=F32)


def head_masks(length):
    lane = lax.broadcasted_iota(jnp.int32, (length, PAIR), 1)
    return lane


def masked_keys(k2, lane, head, valid):
    inside = (lane // HD) == head
    slot = lane == (1 - head) * HD
    row = lax.broadcasted_iota(jnp.int32, lane.shape, 0)
    bias = jnp.where(row < valid, 0.0, -1e30).astype(BF)
    return jnp.where(inside, k2, jnp.where(slot, bias, jnp.zeros_like(k2)))


def masked_query(q2, lane, head):
    inside = (lane // HD) == head
    slot = lane == (1 - head) * HD
    return jnp.where(inside, q2, jnp.where(slot, jnp.ones_like(q2), jnp.zeros_like(q2)))


def attention_forward_kernel(chunk, len_ref, q_ref, k_ref, v_ref, ctx_ref, lse_ref):
    valid = len_ref[pl.program_id(0)]
    length = q_ref.shape[0]
    lane = head_masks(length)
    first_c = lax.broadcasted_iota(jnp.int32, (chunk, PAIR), 1) < HD
    lane_c = lax.broadcasted_iota(jnp.int32, (chunk, PAIR), 1)
    k2, v2 = k_ref[...], v_ref[...]
    km = [masked_keys(k2, lane, h, valid) for h in (0, 1)]
    vm = [jnp.where((lane // HD) == h, v2, jnp.ones_like(v2)) for h in (0, 1)]
    for c in range(length // chunk):
        rows = pl.ds(c * chunk, chunk)
        q2 = q_ref[rows, :] * BF(0.125)
        outs, tops = [], []
        for h in (0, 1):
            s = nt(masked_query(q2, lane_c, h), km[h])
            top = jnp.max(s, axis=1, keepdims=True)
            e = jnp.exp(s - top).astype(BF)
            outs.append(nn(e, vm[h]))
            tops.append(top)
        num = jnp.where(first_c, outs[0], outs[1])
        den = pltpu.roll(jnp.where(first_c, outs[1], outs[0]), HD, 1)
        ctx_ref[rows, :] = (num / den).astype(BF)
        lse = jnp.where(first_c, tops[0], tops[1]) + jnp.log(den)
        turned = lse.T
        lse_ref[0, 0, 0:1, rows] = turned[0:1]
        lse_ref[0, 0, 1:2, rows] = turned[HD : HD + 1]


def attention_forward(lengths, qkv, seqs, length, width, chunk=512):
    pairs = width // PAIR
    return pl.pallas_call(
        functools.partial(attention_forward_kernel, chunk),
        grid_spec=pltpu.PrefetchScalarGridSpec(
            num_scalar_prefetch=1,
            grid=(seqs, pairs),
            in_specs=[
                pl.BlockSpec((length, PAIR), lambda s, p, n: (s, p)),
                pl.BlockSpec((length, PAIR), lambda s, p, n: (s, pairs + p)),
                pl.BlockSpec((length, PAIR), lambda s, p, n: (s, 2 * pairs + p)),
            ],
            out_specs=[
                pl.BlockSpec((length, PAIR), lambda s, p, n: (s, p)),
                pl.BlockSpec((1, 1, 2, length), lambda s, p, n: (s, p, 0, 0)),
            ],
        ),
        out_shape=[
            jax.ShapeDtypeStruct((seqs * length, width), BF),
            jax.ShapeDtypeStruct((seqs, pairs, 2, length), F32),
        ],
        name="attention_forward",
    )(lengths, qkv, qkv, qkv)


def attention_backward_kernel(chunk, len_ref, q_ref, k_ref, v_ref, g_ref, ctx_ref, lse_ref, dq_ref, dk_ref, dv_ref):
    valid = len_ref[pl.program_id(0)]
    length = q_ref.shape[0]
    lane = head_masks(length)
    first = lane < HD
    q2 = q_ref[...] * BF(0.125)
    g2 = g_ref[...]
    k2, v2 = k_ref[...], v_ref[...]
    k8 = k2 * BF(0.125)
    turned = (g2.astype(F32) * ctx_ref[...].astype(F32)).T
    dqs, dks, dvs = [], [], []
    for h in (0, 1):
        km = masked_keys(k2, lane, h, valid)
        qm = masked_query(q2, lane, h)
        vm = jnp.where((lane // HD) == h, v2, jnp.zeros_like(v2))
        delta = jnp.sum(turned[h * HD : (h + 1) * HD], axis=0, keepdims=True)
        lse = lse_ref[0, 0, h : h + 1, :]
        dk_parts, dv_parts, dq = [], [], None
        for c in range(length // chunk):
            rows = slice(c * chunk, (c + 1) * chunk)
            p = jnp.exp(nt(km[rows], qm) - lse)
            ds = (p * (nt(vm[rows], g2) - delta)).astype(BF)
            dv_parts.append(nn(p.astype(BF), g2))
            dk_parts.append(nn(ds, q2))
            part = tn(ds, k8[rows])
            dq = part if dq is None else dq + part
        dqs.append(dq)
        dks.append(jnp.concatenate(dk_parts, 0))
        dvs.append(jnp.concatenate(dv_parts, 0))
    dq_ref[...] = jnp.where(first, dqs[0], dqs[1]).astype(BF)
    dk_ref[...] = jnp.where(first, dks[0], dks[1]).astype(BF)
    dv_ref[...] = jnp.where(first, dvs[0], dvs[1]).astype(BF)


def attention_backward(lengths, qkv, grad, ctx, lse, seqs, length, width, chunk=512):
    pairs = width // PAIR
    col = lambda k: pl.BlockSpec((length, PAIR), lambda s, p, n: (s, k * pairs + p))
    return pl.pallas_call(
        functools.partial(attention_backward_kernel, chunk),
        grid_spec=pltpu.PrefetchScalarGridSpec(
            num_scalar_prefetch=1,
            grid=(seqs, pairs),
            in_specs=[col(0), col(1), col(2), col(0), col(0), pl.BlockSpec((1, 1, 2, length), lambda s, p, n: (s, p, 0, 0))],
            out_specs=[col(0), col(0), col(0)],
        ),
        out_shape=[jax.ShapeDtypeStruct((seqs * length, width), BF)] * 3,
        name="attention_backward",
    )(lengths, qkv, qkv, qkv, grad, ctx, lse)


def gather(mesh_shape, pieces):
    return gather_native(pieces)


def reduce(mesh_shape, terms):
    return reduce_native(terms)


EPS = 1e-06
AXES = ("fsdp", "rep")


def norm_forward(hidden, gain, shift):
    mean = jnp.mean(hidden, axis=-1, keepdims=True)
    centred = hidden - mean
    inverse = lax.rsqrt(jnp.mean(centred * centred, axis=-1, keepdims=True) + EPS)
    normed = centred * inverse
    return (normed * gain + shift, normed, inverse)


def norm_backward(grad_out, normed, inverse, gain):
    grad_normed = grad_out * gain
    grad_in = inverse * (
        grad_normed
        - jnp.mean(grad_normed, axis=-1, keepdims=True)
        - normed * jnp.mean(grad_normed * normed, axis=-1, keepdims=True)
    )
    return (grad_in, jnp.sum(grad_out * normed, axis=0), jnp.sum(grad_out, axis=0))


def column_sums(grad):
    return jnp.sum(grad.astype(F32), axis=0)


def gather_native(pieces):
    return [lax.all_gather(p, AXES, axis=0, tiled=False) for p in pieces]


def reduce_native(terms):
    return [lax.psum_scatter(t.astype(F32), AXES, scatter_dimension=0, tiled=False) for t in terms]


def local(
    mesh_shape,
    hidden_in,
    lengths,
    query_weight,
    key_weight,
    value_weight,
    out_weight,
    up_weight,
    down_weight,
    query_bias,
    value_bias,
    out_bias,
    up_bias,
    down_bias,
    first_gain,
    first_shift,
    second_gain,
    second_shift,
    cotangent,
):
    seqs, length, width = hidden_in.shape
    rows = seqs * length
    hidden = up_weight.shape[1]
    share = query_weight.shape[0]
    spread = hidden // width
    devices = width // share
    vectors = jnp.concatenate(
        [
            jnp.stack([query_bias, value_bias, out_bias, down_bias, first_gain, first_shift, second_gain, second_shift]),
            up_bias.reshape(spread, share),
        ]
    )
    count = vectors.shape[0]
    vector_slot = jnp.pad(vectors, ((0, -count % 16), (0, -share % 128)))
    qkv_shard = jnp.concatenate([query_weight, key_weight, value_weight], axis=1)
    got = gather(mesh_shape, [vector_slot, qkv_shard, out_weight, up_weight, down_weight])
    w_qkv = got[1].reshape(width, 3 * width)
    w_out = got[2].reshape(width, width)
    w_up = got[3].reshape(width, hidden)
    w_down = got[4].reshape(hidden, width)
    wide = got[0].astype(F32)
    plain = jnp.transpose(wide[:, :8, :share], (1, 0, 2)).reshape(8, width)
    b_query, b_values, b_out, b_down, gain_one, shift_one, gain_two, shift_two = [plain[i] for i in range(8)]
    b_up = wide[:, 8 : 8 + spread, :share].reshape(hidden)

    inputs = hidden_in.reshape(rows, width)
    b_qkv = jnp.concatenate([b_query, jnp.zeros_like(b_query), b_values])
    qkv = (nn(inputs, w_qkv) + b_qkv).astype(BF)
    context, log_sums = attention_forward(lengths, qkv, seqs, length, width)
    first_sum = inputs.astype(F32) + nn(context, w_out) + b_out
    first, normed_one, inverse_one = norm_forward(first_sum, gain_one, shift_one)
    first_low = first.astype(BF)
    inner = nn(first_low, w_up) + b_up
    half = 0.5 * (1.0 + lax.erf(inner * (2.0**-0.5)))
    active = (inner * half).astype(BF)
    slope = half + inner * ((2.0 * math.pi) ** -0.5) * jnp.exp(-0.5 * inner * inner)
    slope = slope.astype(BF)
    second_sum = first + nn(active, w_down) + b_down
    result, normed_two, inverse_two = norm_forward(second_sum, gain_two, shift_two)
    hidden_out = result.astype(BF).reshape(seqs, length, width)
    grad_out = cotangent.reshape(rows, width).astype(F32)
    grad_second, grad_gain_two, grad_shift_two = norm_backward(grad_out, normed_two, inverse_two, gain_two)
    grad_branch = grad_second.astype(BF)
    grad_b_down = column_sums(grad_branch)
    grad_w_down = tn(active, grad_branch)
    grad_active = nt(grad_branch, w_down)
    grad_inner = (grad_active * slope.astype(F32)).astype(BF)
    grad_b_up = column_sums(grad_inner)
    grad_w_up = tn(first_low, grad_inner)
    grad_first = grad_second + nt(grad_inner, w_up)
    grad_first_sum, grad_gain_one, grad_shift_one = norm_backward(grad_first, normed_one, inverse_one, gain_one)
    grad_attn = grad_first_sum.astype(BF)
    grad_b_out = column_sums(grad_attn)
    grad_w_out = tn(context, grad_attn)
    grad_context = nt(grad_attn, w_out).astype(BF)
    grad_query, grad_keys, grad_values = attention_backward(
        lengths, qkv, grad_context, context, log_sums, seqs, length, width
    )
    grad_qkv = jnp.concatenate([grad_query, grad_keys, grad_values], axis=1)
    input_grad = (grad_first_sum + nt(grad_qkv, w_qkv)).astype(BF).reshape(seqs, length, width)
    grad_w_qkv = tn(inputs, grad_qkv)
    sums = jnp.stack(
        [
            column_sums(grad_query),
            column_sums(grad_values),
            grad_b_out,
            grad_b_down,
            grad_gain_one,
            grad_shift_one,
            grad_gain_two,
            grad_shift_two,
        ]
    )
    vector_terms = jnp.concatenate(
        [jnp.transpose(sums.reshape(8, devices, share), (1, 0, 2)), grad_b_up.reshape(devices, spread, share)], axis=1
    )
    vector_terms = jnp.pad(vector_terms, ((0, 0), (0, -count % 16), (0, -share % 128)))
    owned = reduce(
        mesh_shape,
        [
            vector_terms,
            grad_w_qkv.reshape(devices, share, 3 * width),
            grad_w_out.reshape(devices, share, width),
            grad_w_up.reshape(devices, share, hidden),
            grad_w_down.reshape(devices, spread * share, width),
        ],
    )
    vec = owned[0][:count, :share]
    return (
        hidden_out,
        input_grad,
        owned[1][:, :width],
        owned[1][:, width : 2 * width],
        owned[1][:, 2 * width :],
        owned[2],
        owned[3],
        owned[4],
        vec[0],
        vec[1],
        vec[2],
        vec[8:].reshape(spread * share),
        vec[3],
        vec[4],
        vec[5],
        vec[6],
        vec[7],
    )


def solution(mesh):
    rows = P(AXES, None)
    flat = P(AXES)
    cube = P(AXES, None, None)
    in_specs = (cube, flat) + (rows,) * 6 + (flat,) * 9 + (cube,)
    out_specs = (cube, cube) + (rows,) * 6 + (flat,) * 9
    body = functools.partial(local, dict(mesh.shape))
    return jax.shard_map(body, mesh=mesh, in_specs=in_specs, out_specs=out_specs, check_vma=False)
```

```python
import functools
import math

import jax
import jax.numpy as jnp
from jax import lax
from jax.experimental import pallas as pl
from jax.experimental.pallas import tpu as pltpu
from jax.sharding import PartitionSpec as P

HD = 64
PAIR = 2 * HD
BF = jnp.bfloat16
F32 = jnp.float32


def nt(left, right):
    return lax.dot_general(left, right, (((1,), (1,)), ((), ())), preferred_element_type=F32)


def nn(left, right):
    return jnp.dot(left, right, preferred_element_type=F32)


def tn(left, right):
    return lax.dot_general(left, right, (((0,), (0,)), ((), ())), preferred_element_type=F32)


def head_masks(length):
    lane = lax.broadcasted_iota(jnp.int32, (length, PAIR), 1)
    return lane


def masked_keys(k2, lane, head, valid):
    inside = (lane // HD) == head
    slot = lane == (1 - head) * HD
    row = lax.broadcasted_iota(jnp.int32, lane.shape, 0)
    bias = jnp.where(row < valid, 0.0, -1e30).astype(BF)
    return jnp.where(inside, k2, jnp.where(slot, bias, jnp.zeros_like(k2)))


def masked_query(q2, lane, head):
    inside = (lane // HD) == head
    slot = lane == (1 - head) * HD
    return jnp.where(inside, q2, jnp.where(slot, jnp.ones_like(q2), jnp.zeros_like(q2)))


def attention_forward_kernel(chunk, len_ref, q_ref, k_ref, v_ref, ctx_ref, lse_ref):
    valid = len_ref[pl.program_id(0)]
    length = q_ref.shape[0]
    lane = head_masks(length)
    first_c = lax.broadcasted_iota(jnp.int32, (chunk, PAIR), 1) < HD
    lane_c = lax.broadcasted_iota(jnp.int32, (chunk, PAIR), 1)
    k2, v2 = k_ref[...], v_ref[...]
    km = [masked_keys(k2, lane, h, valid) for h in (0, 1)]
    vm = [jnp.where((lane // HD) == h, v2, jnp.ones_like(v2)) for h in (0, 1)]
    for c in range(length // chunk):
        rows = pl.ds(c * chunk, chunk)
        q2 = q_ref[rows, :] * BF(0.125)
        outs, tops = [], []
        for h in (0, 1):
            s = nt(masked_query(q2, lane_c, h), km[h])
            top = jnp.max(s, axis=1, keepdims=True)
            e = jnp.exp(s - top).astype(BF)
            outs.append(nn(e, vm[h]))
            tops.append(top)
        num = jnp.where(first_c, outs[0], outs[1])
        den = pltpu.roll(jnp.where(first_c, outs[1], outs[0]), HD, 1)
        ctx_ref[rows, :] = (num / den).astype(BF)
        lse = jnp.where(first_c, tops[0], tops[1]) + jnp.log(den)
        turned = lse.T
        lse_ref[0, 0, 0:1, rows] = turned[0:1]
        lse_ref[0, 0, 1:2, rows] = turned[HD : HD + 1]


def attention_forward(lengths, qkv, seqs, length, width, chunk=512):
    pairs = width // PAIR
    return pl.pallas_call(
        functools.partial(attention_forward_kernel, chunk),
        grid_spec=pltpu.PrefetchScalarGridSpec(
            num_scalar_prefetch=1,
            grid=(seqs, pairs),
            in_specs=[
                pl.BlockSpec((length, PAIR), lambda s, p, n: (s, p)),
                pl.BlockSpec((length, PAIR), lambda s, p, n: (s, pairs + p)),
                pl.BlockSpec((length, PAIR), lambda s, p, n: (s, 2 * pairs + p)),
            ],
            out_specs=[
                pl.BlockSpec((length, PAIR), lambda s, p, n: (s, p)),
                pl.BlockSpec((1, 1, 2, length), lambda s, p, n: (s, p, 0, 0)),
            ],
        ),
        out_shape=[
            jax.ShapeDtypeStruct((seqs * length, width), BF),
            jax.ShapeDtypeStruct((seqs, pairs, 2, length), F32),
        ],
        name="attention_forward",
    )(lengths, qkv, qkv, qkv)


def attention_backward_kernel(chunk, len_ref, q_ref, k_ref, v_ref, g_ref, ctx_ref, lse_ref, dq_ref, dk_ref, dv_ref):
    valid = len_ref[pl.program_id(0)]
    length = q_ref.shape[0]
    lane = head_masks(length)
    first = lane < HD
    q2 = q_ref[...] * BF(0.125)
    g2 = g_ref[...]
    k2, v2 = k_ref[...], v_ref[...]
    k8 = k2 * BF(0.125)
    turned = (g2.astype(F32) * ctx_ref[...].astype(F32)).T
    dqs, dks, dvs = [], [], []
    for h in (0, 1):
        km = masked_keys(k2, lane, h, valid)
        qm = masked_query(q2, lane, h)
        vm = jnp.where((lane // HD) == h, v2, jnp.zeros_like(v2))
        delta = jnp.sum(turned[h * HD : (h + 1) * HD], axis=0, keepdims=True)
        lse = lse_ref[0, 0, h : h + 1, :]
        dk_parts, dv_parts, dq = [], [], None
        for c in range(length // chunk):
            rows = slice(c * chunk, (c + 1) * chunk)
            p = jnp.exp(nt(km[rows], qm) - lse)
            ds = (p * (nt(vm[rows], g2) - delta)).astype(BF)
            dv_parts.append(nn(p.astype(BF), g2))
            dk_parts.append(nn(ds, q2))
            part = tn(ds, k8[rows])
            dq = part if dq is None else dq + part
        dqs.append(dq)
        dks.append(jnp.concatenate(dk_parts, 0))
        dvs.append(jnp.concatenate(dv_parts, 0))
    dq_ref[...] = jnp.where(first, dqs[0], dqs[1]).astype(BF)
    dk_ref[...] = jnp.where(first, dks[0], dks[1]).astype(BF)
    dv_ref[...] = jnp.where(first, dvs[0], dvs[1]).astype(BF)


def attention_backward(lengths, qkv, grad, ctx, lse, seqs, length, width, chunk=512):
    pairs = width // PAIR
    col = lambda k: pl.BlockSpec((length, PAIR), lambda s, p, n: (s, k * pairs + p))
    return pl.pallas_call(
        functools.partial(attention_backward_kernel, chunk),
        grid_spec=pltpu.PrefetchScalarGridSpec(
            num_scalar_prefetch=1,
            grid=(seqs, pairs),
            in_specs=[col(0), col(1), col(2), col(0), col(0), pl.BlockSpec((1, 1, 2, length), lambda s, p, n: (s, p, 0, 0))],
            out_specs=[col(0), col(0), col(0)],
        ),
        out_shape=[jax.ShapeDtypeStruct((seqs * length, width), BF)] * 3,
        name="attention_backward",
    )(lengths, qkv, qkv, qkv, grad, ctx, lse)


def neighbours():
    f, z = lax.axis_index("fsdp"), lax.axis_index("rep")
    core, x, y = f % 2, (f // 2) % 2, f // 4
    across_core = f + 1 - 2 * core
    step_x, step_y = 2 * (1 - 2 * x), 4 * (1 - 2 * y)
    return f, z, across_core, step_x, step_y


def remote(src, dst, send_sem, recv_sem, device):
    return pltpu.make_async_remote_copy(
        src_ref=src,
        dst_ref=dst,
        send_sem=send_sem,
        recv_sem=recv_sem,
        device_id=device,
        device_id_type=pl.DeviceIdType.MESH,
    )


def meet(depth, f, z, across_core, step_x, step_y):
    barrier = pltpu.get_barrier_semaphore()

    def greet(device):
        pl.semaphore_signal(barrier, inc=1, device_id=device, device_id_type=pl.DeviceIdType.MESH)

    for other in (across_core, f + step_x, f + step_y):
        greet((other, z))

    @pl.when(z > 0)
    def _():
        greet((f, z - 1))

    @pl.when(z < depth - 1)
    def _():
        greet((f, z + 1))

    pl.semaphore_wait(barrier, 3 + jnp.minimum(z, 1) + jnp.minimum(depth - 1 - z, 1))


def far_first(step, z):
    zero = 3 * (1 - z // 2)
    one = (2 + 3 * z) % 5
    two = 1 + z % 2
    picks = (zero, one, two, z)
    total = 0
    for i, pick in enumerate(picks):
        hit = 1 - jnp.minimum(jnp.abs(step - i), 1)
        total = total + hit * pick
    return total


def strips_of(arrays):
    found = []
    for index, array in enumerate(arrays):
        columns = array[1]
        if columns % 256 == 0 and columns >= 2304 and index == 1:
            found.append((index, 0, columns // 2, True))
            found.append((index, columns // 2, columns // 2, False))
        else:
            found.append((index, 0, None, index in (2, 3)))
    return found


def cut(ref, strip):
    if strip[2] is None:
        return ref
    return ref.at[:, pl.ds(strip[1], strip[2])]


def gather_kernel(depth, strips, count, *refs):
    ins, outs, sems = refs[:count], refs[count : 2 * count], refs[2 * count :]
    (own_sem, up_sem, down_sem, first_sem, second_sem, relay_sem, core_sem) = sems[:7]
    (got_column, got_first, got_second, got_diagonal, got_core) = sems[7:]
    f, z, across_core, step_x, step_y = neighbours()
    meet(depth, f, z, across_core, step_x, step_y)

    def slot(who, plane):
        return who * depth + plane

    def place(n, who, plane):
        return cut(outs[strips[n][0]].at[slot(who, plane)], strips[n])

    def toward(n):
        return (step_x, step_y) if strips[n][3] else (step_y, step_x)

    def own_copy(a):
        return pltpu.make_async_copy(ins[a], outs[a].at[slot(f, z)], own_sem.at[a])

    def core_copy(n, kind, plane, src):
        first, second = toward(n)
        who = f + (0, first, second, first + second)[kind]
        where = place(n, who, plane)
        return remote(where if src is None else src, where, core_sem.at[n, kind, plane], got_core.at[n, kind, plane], (across_core, z))

    def core_arrival(n, kind, plane):
        first, second = toward(n)
        who = across_core + (0, first, second, first + second)[kind]
        where = place(n, who, plane)
        return remote(where, where, core_sem.at[n, kind, plane], got_core.at[n, kind, plane], (across_core, z))

    def column_up(n, plane, src):
        return remote(src, place(n, f, plane), up_sem.at[n, plane], got_column.at[n, plane], (f, z + 1))

    def column_down(n, plane, src):
        return remote(src, place(n, f, plane), down_sem.at[n, plane], got_column.at[n, plane], (f, z - 1))

    def to_first(n, plane, src):
        return remote(src, place(n, f, plane), first_sem.at[n, plane], got_first.at[n, plane], (f + toward(n)[0], z))

    def to_second(n, plane, src):
        return remote(src, place(n, f, plane), second_sem.at[n, plane], got_second.at[n, plane], (f + toward(n)[1], z))

    def relay(n, plane):
        where = place(n, f + toward(n)[0], plane)
        return remote(where, where, relay_sem.at[n, plane], got_diagonal.at[n, plane], (f + toward(n)[1], z))

    def each(body):
        for n in range(len(strips)):
            body(n)

    for a in range(count):
        own_copy(a).start()

    def send_own(n):
        src = cut(ins[strips[n][0]], strips[n])
        to_first(n, z, src).start()
        to_second(n, z, src).start()

        @pl.when(z < depth - 1)
        def _():
            column_up(n, z, src).start()

        @pl.when(z > 0)
        def _():
            column_down(n, z, src).start()

        core_copy(n, 0, z, src).start()

    each(send_own)

    def step(t, carry):
        plane = far_first(depth - 1 - t, z)
        before = far_first(depth - t, z)
        earlier = far_first(depth + 1 - t, z)

        @pl.when((t >= 1) & (t < depth))
        def _():
            def arrived(n):
                src = place(n, f, plane)
                remote(src, src, up_sem.at[n, plane], got_column.at[n, plane], (f, z)).wait_recv()
                to_first(n, plane, src).start()
                to_second(n, plane, src).start()

                @pl.when((plane < z) & (z < depth - 1))
                def _():
                    column_up(n, plane, src).start()

                @pl.when((plane > z) & (z > 0))
                def _():
                    column_down(n, plane, src).start()

                core_copy(n, 0, plane, None).start()

            each(arrived)

        @pl.when((t >= 1) & (t < depth + 1))
        def _():
            def beside(n):
                first, second = toward(n)
                here = place(n, f + first, before)
                remote(here, here, first_sem.at[n, before], got_first.at[n, before], (f + first, z)).wait_recv()
                relay(n, before).start()
                core_copy(n, 1, before, None).start()

            each(beside)

            def above(n):
                first, second = toward(n)
                here = place(n, f + second, before)
                remote(here, here, second_sem.at[n, before], got_second.at[n, before], (f + second, z)).wait_recv()
                core_copy(n, 2, before, None).start()

            each(above)

        @pl.when(t >= 2)
        def _():
            def opposite(n):
                first, second = toward(n)
                here = place(n, f + first + second, earlier)
                remote(here, here, relay_sem.at[n, earlier], got_diagonal.at[n, earlier], (f + second, z)).wait_recv()
                core_copy(n, 3, earlier, None).start()

            each(opposite)

        return carry

    lax.fori_loop(0, depth + 2, step, 0)

    for a in range(count):
        own_copy(a).wait()

    def finish(plane, carry):
        def close(n):
            src = place(n, f, plane)
            to_first(n, plane, src).wait_send()
            to_second(n, plane, src).wait_send()
            relay(n, plane).wait_send()

            @pl.when((plane <= z) & (z < depth - 1))
            def _():
                column_up(n, plane, src).wait_send()

            @pl.when((plane >= z) & (z > 0))
            def _():
                column_down(n, plane, src).wait_send()

            for kind in range(4):
                core_copy(n, kind, plane, None).wait_send()
                core_arrival(n, kind, plane).wait_recv()

        each(close)
        return carry

    lax.fori_loop(0, depth, finish, 0)


def gather_remote(mesh_shape, pieces):
    depth, devices = mesh_shape["rep"], mesh_shape["rep"] * mesh_shape["fsdp"]
    strips = strips_of([p.shape for p in pieces])
    count, n = len(pieces), len(strips)
    dma = pltpu.SemaphoreType.DMA
    flat, cored = dma((n, depth)), dma((n, 4, depth))
    return pl.pallas_call(
        functools.partial(gather_kernel, depth, strips, count),
        out_shape=[jax.ShapeDtypeStruct((devices,) + p.shape, p.dtype) for p in pieces],
        in_specs=[pl.BlockSpec(memory_space=pltpu.VMEM)] * count,
        out_specs=[pl.BlockSpec(memory_space=pl.ANY)] * count,
        scratch_shapes=[dma((count,)), flat, flat, flat, flat, flat, cored, flat, flat, flat, flat, cored],
        compiler_params=pltpu.CompilerParams(collective_id=1, has_side_effects=True),
        name="gather_weights",
    )(*pieces)


def fits(mesh_shape, share):
    return mesh_shape["fsdp"] == 8 and mesh_shape["rep"] == 4 and share % 8 == 0


def gather(mesh_shape, pieces):
    if fits(mesh_shape, pieces[1].shape[0]):
        return gather_remote(mesh_shape, pieces)
    return gather_native(pieces)


def reduce_kernel(depth, strips, count, *refs):
    terms, outs = refs[:count], refs[count : 2 * count]
    mine, theirs = refs[2 * count : 3 * count], refs[3 * count : 4 * count]
    relayed, direct, partial, below, above = (refs[(4 + i) * count : (5 + i) * count] for i in range(5))
    sems = refs[9 * count :]
    (own_sem, core_sem, relay_sem, direct_sem, partial_sem, up_sem, down_sem) = sems[:7]
    (got_core, got_relay, got_direct, got_partial, got_below, got_above) = sems[7:]
    f, z, across_core, step_x, step_y = neighbours()
    meet(depth, f, z, across_core, step_x, step_y)

    def toward(n):
        return (step_x, step_y) if strips[n][3] else (step_y, step_x)

    def steps(n):
        first, second = toward(n)
        return (0, first, second, first + second)

    def term(n, who, plane):
        return cut(terms[strips[n][0]].at[who * depth + plane], strips[n])

    def cell(family, n, *index):
        return cut(family[strips[n][0]].at[index], strips[n])

    def own_copy(n, kind, plane):
        return pltpu.make_async_copy(term(n, f + steps(n)[kind], plane), cell(mine, n, kind, plane), own_sem.at[n, kind, plane])

    def core_copy(n, kind, plane):
        return remote(
            term(n, across_core + steps(n)[kind], plane),
            cell(theirs, n, kind, plane),
            core_sem.at[n, kind, plane],
            got_core.at[n, kind, plane],
            (across_core, z),
        )

    def relay(n, plane):
        return remote(cell(theirs, n, 3, plane), cell(relayed, n, plane), relay_sem.at[n, plane], got_relay.at[n, plane], (f + toward(n)[1], z))

    def straight(n, plane):
        return remote(cell(theirs, n, 2, plane), cell(direct, n, plane), direct_sem.at[n, plane], got_direct.at[n, plane], (f + toward(n)[1], z))

    def second_hop(n, plane):
        return remote(cell(theirs, n, 1, plane), cell(partial, n, plane), partial_sem.at[n, plane], got_partial.at[n, plane], (f + toward(n)[0], z))

    def go_up(n, plane):
        return remote(cell(theirs, n, 0, plane), cell(below, n, plane), up_sem.at[n, plane], got_below.at[n, plane], (f, z + 1))

    def go_down(n, plane):
        return remote(cell(theirs, n, 0, plane), cell(above, n, plane), down_sem.at[n, plane], got_above.at[n, plane], (f, z - 1))

    def add(n, kind, plane, *others):
        here = cell(theirs, n, kind, plane)
        total = here[...].astype(F32)
        for other in others:
            total = total + other[...].astype(F32)
        here[...] = total.astype(here.dtype)

    each = range(len(strips))
    order = (3, 2, 1, 0)

    def launch(t, carry):
        plane = far_first(t, z)
        for kind in order:
            for n in each:
                core_copy(n, kind, plane).start()
                own_copy(n, kind, plane).start()
        return carry

    lax.fori_loop(0, depth, launch, 0)

    def step(t, carry):
        plane = far_first(t, z)
        before = far_first(t - 1, z)
        earlier = far_first(t - 2, z)

        @pl.when(t < depth)
        def _():
            for kind in order:
                for n in each:
                    core_copy(n, kind, plane).wait_recv()
                    own_copy(n, kind, plane).wait()
                    add(n, kind, plane, cell(mine, n, kind, plane))
                if kind == 3:
                    for n in each:
                        relay(n, plane).start()
                if kind == 2:
                    for n in each:
                        straight(n, plane).start()

        @pl.when((t >= 1) & (t < depth + 1))
        def _():
            for n in each:
                relay(n, before).wait_recv()
                add(n, 1, before, cell(relayed, n, before))
            for n in each:
                second_hop(n, before).start()

        @pl.when(t >= 2)
        def _():
            for n in each:
                straight(n, earlier).wait_recv()
                second_hop(n, earlier).wait_recv()
                add(n, 0, earlier, cell(direct, n, earlier), cell(partial, n, earlier))

            @pl.when((earlier >= z) & (z > 0))
            def _():
                for n in each:
                    go_up(n, earlier).wait_recv()
                    add(n, 0, earlier, cell(below, n, earlier))

            @pl.when((earlier <= z) & (z < depth - 1))
            def _():
                for n in each:
                    go_down(n, earlier).wait_recv()
                    add(n, 0, earlier, cell(above, n, earlier))

            @pl.when(earlier > z)
            def _():
                for n in each:
                    go_up(n, earlier).start()

            @pl.when(earlier < z)
            def _():
                for n in each:
                    go_down(n, earlier).start()

        return carry

    lax.fori_loop(0, depth + 2, step, 0)
    for a in range(count):
        outs[a][...] = theirs[a][0, z].astype(F32)

    def finish(plane, carry):
        for n in each:
            for kind in order:
                core_copy(n, kind, plane).wait_send()
            relay(n, plane).wait_send()
            straight(n, plane).wait_send()
            second_hop(n, plane).wait_send()

        @pl.when(plane > z)
        def _():
            for n in each:
                go_up(n, plane).wait_send()

        @pl.when(plane < z)
        def _():
            for n in each:
                go_down(n, plane).wait_send()

        return carry

    lax.fori_loop(0, depth, finish, 0)


def reduce_remote(mesh_shape, terms, collective_id=2):
    depth = mesh_shape["rep"]
    strips = strips_of([t.shape[1:] for t in terms])
    count, n = len(terms), len(strips)
    dma = pltpu.SemaphoreType.DMA
    flat, cored = dma((n, depth)), dma((n, 4, depth))
    whole = [pltpu.VMEM((4, depth) + t.shape[1:], t.dtype) for t in terms]
    line = [pltpu.VMEM((depth,) + t.shape[1:], t.dtype) for t in terms]
    return pl.pallas_call(
        functools.partial(reduce_kernel, depth, strips, count),
        out_shape=[jax.ShapeDtypeStruct(t.shape[1:], F32) for t in terms],
        in_specs=[pl.BlockSpec(memory_space=pl.ANY)] * count,
        out_specs=[pl.BlockSpec(memory_space=pltpu.VMEM)] * count,
        scratch_shapes=whole + whole + line * 5 + [cored, cored, flat, flat, flat, flat, flat, cored, flat, flat, flat, flat, flat],
        compiler_params=pltpu.CompilerParams(
            collective_id=collective_id, has_side_effects=True, vmem_limit_bytes=48 * 1024 * 1024
        ),
        name="reduce_terms",
    )(*terms)


def reduce(mesh_shape, terms):
    if fits(mesh_shape, terms[1].shape[1]):
        return reduce_remote(mesh_shape, [t.astype(F32 if i == 0 else BF) for i, t in enumerate(terms)])
    return reduce_native(terms)


EPS = 1e-06
AXES = ("fsdp", "rep")


def norm_forward(hidden, gain, shift):
    mean = jnp.mean(hidden, axis=-1, keepdims=True)
    centred = hidden - mean
    inverse = lax.rsqrt(jnp.mean(centred * centred, axis=-1, keepdims=True) + EPS)
    normed = centred * inverse
    return (normed * gain + shift, normed, inverse)


def norm_backward(grad_out, normed, inverse, gain):
    grad_normed = grad_out * gain
    grad_in = inverse * (
        grad_normed
        - jnp.mean(grad_normed, axis=-1, keepdims=True)
        - normed * jnp.mean(grad_normed * normed, axis=-1, keepdims=True)
    )
    return (grad_in, jnp.sum(grad_out * normed, axis=0), jnp.sum(grad_out, axis=0))


def column_sums(grad):
    return jnp.sum(grad.astype(F32), axis=0)


def gather_native(pieces):
    return [lax.all_gather(p, AXES, axis=0, tiled=False) for p in pieces]


def reduce_native(terms):
    return [lax.psum_scatter(t.astype(F32), AXES, scatter_dimension=0, tiled=False) for t in terms]


def local(
    mesh_shape,
    hidden_in,
    lengths,
    query_weight,
    key_weight,
    value_weight,
    out_weight,
    up_weight,
    down_weight,
    query_bias,
    value_bias,
    out_bias,
    up_bias,
    down_bias,
    first_gain,
    first_shift,
    second_gain,
    second_shift,
    cotangent,
):
    seqs, length, width = hidden_in.shape
    rows = seqs * length
    hidden = up_weight.shape[1]
    share = query_weight.shape[0]
    spread = hidden // width
    devices = width // share
    vectors = jnp.concatenate(
        [
            jnp.stack([query_bias, value_bias, out_bias, down_bias, first_gain, first_shift, second_gain, second_shift]),
            up_bias.reshape(spread, share),
        ]
    )
    count = vectors.shape[0]
    vector_slot = jnp.pad(vectors, ((0, -count % 16), (0, -share % 128)))
    qkv_shard = jnp.concatenate([query_weight, key_weight, value_weight], axis=1)
    got = gather(mesh_shape, [vector_slot, qkv_shard, out_weight, up_weight, down_weight])
    w_qkv = got[1].reshape(width, 3 * width)
    w_out = got[2].reshape(width, width)
    w_up = got[3].reshape(width, hidden)
    w_down = got[4].reshape(hidden, width)
    wide = got[0].astype(F32)
    plain = jnp.transpose(wide[:, :8, :share], (1, 0, 2)).reshape(8, width)
    b_query, b_values, b_out, b_down, gain_one, shift_one, gain_two, shift_two = [plain[i] for i in range(8)]
    b_up = wide[:, 8 : 8 + spread, :share].reshape(hidden)

    inputs = hidden_in.reshape(rows, width)
    b_qkv = jnp.concatenate([b_query, jnp.zeros_like(b_query), b_values])
    qkv = (nn(inputs, w_qkv) + b_qkv).astype(BF)
    context, log_sums = attention_forward(lengths, qkv, seqs, length, width)
    first_sum = inputs.astype(F32) + nn(context, w_out) + b_out
    first, normed_one, inverse_one = norm_forward(first_sum, gain_one, shift_one)
    first_low = first.astype(BF)
    inner = nn(first_low, w_up) + b_up
    half = 0.5 * (1.0 + lax.erf(inner * (2.0**-0.5)))
    active = (inner * half).astype(BF)
    slope = half + inner * ((2.0 * math.pi) ** -0.5) * jnp.exp(-0.5 * inner * inner)
    slope = slope.astype(BF)
    second_sum = first + nn(active, w_down) + b_down
    result, normed_two, inverse_two = norm_forward(second_sum, gain_two, shift_two)
    hidden_out = result.astype(BF).reshape(seqs, length, width)
    grad_out = cotangent.reshape(rows, width).astype(F32)
    grad_second, grad_gain_two, grad_shift_two = norm_backward(grad_out, normed_two, inverse_two, gain_two)
    grad_branch = grad_second.astype(BF)
    grad_b_down = column_sums(grad_branch)
    grad_w_down = tn(active, grad_branch)
    grad_active = nt(grad_branch, w_down)
    grad_inner = (grad_active * slope.astype(F32)).astype(BF)
    grad_b_up = column_sums(grad_inner)
    grad_w_up = tn(first_low, grad_inner)
    grad_first = grad_second + nt(grad_inner, w_up)
    grad_first_sum, grad_gain_one, grad_shift_one = norm_backward(grad_first, normed_one, inverse_one, gain_one)
    grad_attn = grad_first_sum.astype(BF)
    grad_b_out = column_sums(grad_attn)
    grad_w_out = tn(context, grad_attn)
    grad_context = nt(grad_attn, w_out).astype(BF)
    grad_query, grad_keys, grad_values = attention_backward(
        lengths, qkv, grad_context, context, log_sums, seqs, length, width
    )
    grad_qkv = jnp.concatenate([grad_query, grad_keys, grad_values], axis=1)
    input_grad = (grad_first_sum + nt(grad_qkv, w_qkv)).astype(BF).reshape(seqs, length, width)
    grad_w_qkv = tn(inputs, grad_qkv)
    sums = jnp.stack(
        [
            column_sums(grad_query),
            column_sums(grad_values),
            grad_b_out,
            grad_b_down,
            grad_gain_one,
            grad_shift_one,
            grad_gain_two,
            grad_shift_two,
        ]
    )
    vector_terms = jnp.concatenate(
        [jnp.transpose(sums.reshape(8, devices, share), (1, 0, 2)), grad_b_up.reshape(devices, spread, share)], axis=1
    )
    vector_terms = jnp.pad(vector_terms, ((0, 0), (0, -count % 16), (0, -share % 128)))
    owned = reduce(
        mesh_shape,
        [
            vector_terms,
            grad_w_qkv.reshape(devices, share, 3 * width),
            grad_w_out.reshape(devices, share, width),
            grad_w_up.reshape(devices, share, hidden),
            grad_w_down.reshape(devices, spread * share, width),
        ],
    )
    vec = owned[0][:count, :share]
    return (
        hidden_out,
        input_grad,
        owned[1][:, :width],
        owned[1][:, width : 2 * width],
        owned[1][:, 2 * width :],
        owned[2],
        owned[3],
        owned[4],
        vec[0],
        vec[1],
        vec[2],
        vec[8:].reshape(spread * share),
        vec[3],
        vec[4],
        vec[5],
        vec[6],
        vec[7],
    )


def solution(mesh):
    rows = P(AXES, None)
    flat = P(AXES)
    cube = P(AXES, None, None)
    in_specs = (cube, flat) + (rows,) * 6 + (flat,) * 9 + (cube,)
    out_specs = (cube, cube) + (rows,) * 6 + (flat,) * 9
    body = functools.partial(local, dict(mesh.shape))
    return jax.shard_map(body, mesh=mesh, in_specs=in_specs, out_specs=out_specs, check_vma=False)
```

```python
import functools
import math

import jax
import jax.numpy as jnp
from jax import lax
from jax.experimental import pallas as pl
from jax.experimental.pallas import tpu as pltpu
from jax.sharding import PartitionSpec as P

HD = 64
PAIR = 2 * HD
BF = jnp.bfloat16
F32 = jnp.float32


def nt(left, right):
    return lax.dot_general(left, right, (((1,), (1,)), ((), ())), preferred_element_type=F32)


def nn(left, right):
    return jnp.dot(left, right, preferred_element_type=F32)


def tn(left, right):
    return lax.dot_general(left, right, (((0,), (0,)), ((), ())), preferred_element_type=F32)


def head_masks(length):
    lane = lax.broadcasted_iota(jnp.int32, (length, PAIR), 1)
    return lane


def masked_keys(k2, lane, head, valid):
    inside = (lane // HD) == head
    slot = lane == (1 - head) * HD
    row = lax.broadcasted_iota(jnp.int32, lane.shape, 0)
    bias = jnp.where(row < valid, 0.0, -1e30).astype(BF)
    return jnp.where(inside, k2, jnp.where(slot, bias, jnp.zeros_like(k2)))


def masked_query(q2, lane, head):
    inside = (lane // HD) == head
    slot = lane == (1 - head) * HD
    return jnp.where(inside, q2, jnp.where(slot, jnp.ones_like(q2), jnp.zeros_like(q2)))


def forward_pair(valid, q2, k2, v2):
    lane = head_masks(q2.shape[0])
    first = lane < HD
    q2 = q2 * BF(0.125)
    outs, tops = [], []
    for h in (0, 1):
        s = nt(masked_query(q2, lane, h), masked_keys(k2, lane, h, valid))
        top = jnp.max(s, axis=1, keepdims=True)
        e = jnp.exp(s - top).astype(BF)
        outs.append(nn(e, jnp.where((lane // HD) == h, v2, jnp.ones_like(v2))))
        tops.append(top)
    num = jnp.where(first, outs[0], outs[1])
    den = pltpu.roll(jnp.where(first, outs[1], outs[0]), HD, 1)
    lse = jnp.where(first, tops[0], tops[1]) + jnp.log(den)
    turned = lse.T
    return (num / den).astype(BF), turned[0:1], turned[HD : HD + 1]


def attention_forward_kernel(len_ref, q_ref, k_ref, v_ref, ctx_ref, lse_ref):
    ctx, low, high = forward_pair(len_ref[pl.program_id(0)], q_ref[...], k_ref[...], v_ref[...])
    ctx_ref[...] = ctx
    lse_ref[0, 0, 0:1, :] = low
    lse_ref[0, 0, 1:2, :] = high


def attention_forward(lengths, qkv, seqs, length, width):
    pairs = width // PAIR
    return pl.pallas_call(
        attention_forward_kernel,
        grid_spec=pltpu.PrefetchScalarGridSpec(
            num_scalar_prefetch=1,
            grid=(seqs, pairs),
            in_specs=[
                pl.BlockSpec((length, PAIR), lambda s, p, n: (s, p)),
                pl.BlockSpec((length, PAIR), lambda s, p, n: (s, pairs + p)),
                pl.BlockSpec((length, PAIR), lambda s, p, n: (s, 2 * pairs + p)),
            ],
            out_specs=[
                pl.BlockSpec((length, PAIR), lambda s, p, n: (s, p)),
                pl.BlockSpec((1, 1, 2, length), lambda s, p, n: (s, p, 0, 0)),
            ],
        ),
        out_shape=[
            jax.ShapeDtypeStruct((seqs * length, width), BF),
            jax.ShapeDtypeStruct((seqs, pairs, 2, length), F32),
        ],
        name="attention_forward",
    )(lengths, qkv, qkv, qkv)


def backward_pair(valid, q2, k2, v2, g2, ctx2, lses):
    lane = head_masks(q2.shape[0])
    first = lane < HD
    q2 = q2 * BF(0.125)
    k8 = k2 * BF(0.125)
    turned = (g2.astype(F32) * ctx2.astype(F32)).T
    dqs, dks, dvs = [], [], []
    for h in (0, 1):
        km = masked_keys(k2, lane, h, valid)
        qm = masked_query(q2, lane, h)
        vm = jnp.where((lane // HD) == h, v2, jnp.zeros_like(v2))
        delta = jnp.sum(turned[h * HD : (h + 1) * HD], axis=0, keepdims=True)
        p = jnp.exp(nt(km, qm) - lses[h])
        ds = (p * (nt(vm, g2) - delta)).astype(BF)
        dvs.append(nn(p.astype(BF), g2))
        dks.append(nn(ds, q2))
        dqs.append(tn(ds, k8))
    return [jnp.where(first, pair[0], pair[1]).astype(BF) for pair in (dqs, dks, dvs)]


def attention_backward_kernel(len_ref, q_ref, k_ref, v_ref, g_ref, ctx_ref, lse_ref, dq_ref, dk_ref, dv_ref):
    lses = [lse_ref[0, 0, h : h + 1, :] for h in (0, 1)]
    valid = len_ref[pl.program_id(0)]
    dq_ref[...], dk_ref[...], dv_ref[...] = backward_pair(
        valid, q_ref[...], k_ref[...], v_ref[...], g_ref[...], ctx_ref[...], lses
    )


def attention_backward(lengths, qkv, grad, ctx, lse, seqs, length, width):
    pairs = width // PAIR
    col = lambda k: pl.BlockSpec((length, PAIR), lambda s, p, n: (s, k * pairs + p))
    return pl.pallas_call(
        attention_backward_kernel,
        grid_spec=pltpu.PrefetchScalarGridSpec(
            num_scalar_prefetch=1,
            grid=(seqs, pairs),
            in_specs=[col(0), col(1), col(2), col(0), col(0), pl.BlockSpec((1, 1, 2, length), lambda s, p, n: (s, p, 0, 0))],
            out_specs=[col(0), col(0), col(0)],
        ),
        out_shape=[jax.ShapeDtypeStruct((seqs * length, width), BF)] * 3,
        name="attention_backward",
    )(lengths, qkv, qkv, qkv, grad, ctx, lse)


def neighbours():
    f, z = lax.axis_index("fsdp"), lax.axis_index("rep")
    core, x, y = f % 2, (f // 2) % 2, f // 4
    across_core = f + 1 - 2 * core
    step_x, step_y = 2 * (1 - 2 * x), 4 * (1 - 2 * y)
    return f, z, across_core, step_x, step_y


def remote(src, dst, send_sem, recv_sem, device):
    return pltpu.make_async_remote_copy(
        src_ref=src,
        dst_ref=dst,
        send_sem=send_sem,
        recv_sem=recv_sem,
        device_id=device,
        device_id_type=pl.DeviceIdType.MESH,
    )


def meet(depth, f, z, across_core, step_x, step_y):
    barrier = pltpu.get_barrier_semaphore()

    def greet(device):
        pl.semaphore_signal(barrier, inc=1, device_id=device, device_id_type=pl.DeviceIdType.MESH)

    for other in (across_core, f + step_x, f + step_y):
        greet((other, z))

    @pl.when(z > 0)
    def _():
        greet((f, z - 1))

    @pl.when(z < depth - 1)
    def _():
        greet((f, z + 1))

    pl.semaphore_wait(barrier, 3 + jnp.minimum(z, 1) + jnp.minimum(depth - 1 - z, 1))


def far_first(step, z):
    zero = 3 * (1 - z // 2)
    one = (2 + 3 * z) % 5
    two = 1 + z % 2
    picks = (zero, one, two, z)
    total = 0
    for i, pick in enumerate(picks):
        hit = 1 - jnp.minimum(jnp.abs(step - i), 1)
        total = total + hit * pick
    return total


def strips_of(arrays):
    found = []
    for index, array in enumerate(arrays):
        columns = array[1]
        if columns % 256 == 0:
            found.append((index, 0, columns // 2, True))
            found.append((index, columns // 2, columns // 2, False))
        else:
            found.append((index, 0, None, True))
    return found


def cut(ref, strip):
    if strip[2] is None:
        return ref
    return ref.at[:, pl.ds(strip[1], strip[2])]


def gather_parts(depth, strips, ins, outs, sems):
    count = len(ins)
    (own_sem, up_sem, down_sem, first_sem, second_sem, relay_sem, core_sem) = sems[:7]
    (got_column, got_first, got_second, got_diagonal, got_core) = sems[7:]
    f, z, across_core, step_x, step_y = neighbours()

    def slot(who, plane):
        return who * depth + plane

    def place(n, who, plane):
        return cut(outs[strips[n][0]].at[slot(who, plane)], strips[n])

    def toward(n):
        return (step_x, step_y) if strips[n][3] else (step_y, step_x)

    def own_copy(a):
        return pltpu.make_async_copy(ins[a], outs[a].at[slot(f, z)], own_sem.at[a])

    def core_copy(n, kind, plane, src):
        first, second = toward(n)
        who = f + (0, first, second, first + second)[kind]
        where = place(n, who, plane)
        return remote(where if src is None else src, where, core_sem.at[n, kind, plane], got_core.at[n, kind, plane], (across_core, z))

    def core_arrival(n, kind, plane):
        first, second = toward(n)
        who = across_core + (0, first, second, first + second)[kind]
        where = place(n, who, plane)
        return remote(where, where, core_sem.at[n, kind, plane], got_core.at[n, kind, plane], (across_core, z))

    def column_up(n, plane, src):
        return remote(src, place(n, f, plane), up_sem.at[n, plane], got_column.at[n, plane], (f, z + 1))

    def column_down(n, plane, src):
        return remote(src, place(n, f, plane), down_sem.at[n, plane], got_column.at[n, plane], (f, z - 1))

    def to_first(n, plane, src):
        return remote(src, place(n, f, plane), first_sem.at[n, plane], got_first.at[n, plane], (f + toward(n)[0], z))

    def to_second(n, plane, src):
        return remote(src, place(n, f, plane), second_sem.at[n, plane], got_second.at[n, plane], (f + toward(n)[1], z))

    def relay(n, plane):
        where = place(n, f + toward(n)[0], plane)
        return remote(where, where, relay_sem.at[n, plane], got_diagonal.at[n, plane], (f + toward(n)[1], z))

    def each(body):
        for n in range(len(strips)):
            body(n)

    def send_own(n):
        src = cut(ins[strips[n][0]], strips[n])
        to_first(n, z, src).start()
        to_second(n, z, src).start()

        @pl.when(z < depth - 1)
        def _():
            column_up(n, z, src).start()

        @pl.when(z > 0)
        def _():
            column_down(n, z, src).start()

        core_copy(n, 0, z, src).start()

    def begin():
        meet(depth, f, z, across_core, step_x, step_y)
        for a in range(count):
            own_copy(a).start()
        each(send_own)

    def phase(t):
        plane = far_first(depth - 1 - t, z)
        before = far_first(depth - t, z)
        earlier = far_first(depth + 1 - t, z)

        @pl.when((t >= 1) & (t < depth))
        def _():
            def arrived(n):
                src = place(n, f, plane)
                remote(src, src, up_sem.at[n, plane], got_column.at[n, plane], (f, z)).wait_recv()
                to_first(n, plane, src).start()
                to_second(n, plane, src).start()

                @pl.when((plane < z) & (z < depth - 1))
                def _():
                    column_up(n, plane, src).start()

                @pl.when((plane > z) & (z > 0))
                def _():
                    column_down(n, plane, src).start()

                core_copy(n, 0, plane, None).start()

            each(arrived)

        @pl.when((t >= 1) & (t < depth + 1))
        def _():
            def beside(n):
                first, second = toward(n)
                here = place(n, f + first, before)
                remote(here, here, first_sem.at[n, before], got_first.at[n, before], (f + first, z)).wait_recv()
                relay(n, before).start()
                core_copy(n, 1, before, None).start()

            each(beside)

            def above(n):
                first, second = toward(n)
                here = place(n, f + second, before)
                remote(here, here, second_sem.at[n, before], got_second.at[n, before], (f + second, z)).wait_recv()
                core_copy(n, 2, before, None).start()

            each(above)

        @pl.when(t >= 2)
        def _():
            def opposite(n):
                first, second = toward(n)
                here = place(n, f + first + second, earlier)
                remote(here, here, relay_sem.at[n, earlier], got_diagonal.at[n, earlier], (f + second, z)).wait_recv()
                core_copy(n, 3, earlier, None).start()

            each(opposite)

    def close_plane(plane, carry):
        def close(n):
            src = place(n, f, plane)
            to_first(n, plane, src).wait_send()
            to_second(n, plane, src).wait_send()
            relay(n, plane).wait_send()

            @pl.when((plane <= z) & (z < depth - 1))
            def _():
                column_up(n, plane, src).wait_send()

            @pl.when((plane >= z) & (z > 0))
            def _():
                column_down(n, plane, src).wait_send()

            for kind in range(4):
                core_copy(n, kind, plane, None).wait_send()
                core_arrival(n, kind, plane).wait_recv()

        each(close)
        return carry

    def finish():
        for a in range(count):
            own_copy(a).wait()
        lax.fori_loop(0, depth, close_plane, 0)

    return begin, phase, finish


def gather_kernel(depth, strips, count, *refs):
    ins, outs, sems = refs[:count], refs[count : 2 * count], refs[2 * count :]
    begin, phase, finish = gather_parts(depth, strips, ins, outs, sems)
    begin()

    def step(t, carry):
        phase(t)
        return carry

    lax.fori_loop(1, depth + 2, step, 0)
    finish()


def gather_semaphores(strips, count, depth):
    dma = pltpu.SemaphoreType.DMA
    flat, cored = dma((len(strips), depth)), dma((len(strips), 4, depth))
    return [dma((count,)), flat, flat, flat, flat, flat, cored, flat, flat, flat, flat, cored]


def gather_remote(mesh_shape, pieces):
    depth, devices = mesh_shape["rep"], mesh_shape["rep"] * mesh_shape["fsdp"]
    strips = strips_of([p.shape for p in pieces])
    count = len(pieces)
    return pl.pallas_call(
        functools.partial(gather_kernel, depth, strips, count),
        out_shape=[jax.ShapeDtypeStruct((devices,) + p.shape, p.dtype) for p in pieces],
        in_specs=[pl.BlockSpec(memory_space=pltpu.VMEM)] * count,
        out_specs=[pl.BlockSpec(memory_space=pl.ANY)] * count,
        scratch_shapes=gather_semaphores(strips, count, depth),
        compiler_params=pltpu.CompilerParams(collective_id=1, has_side_effects=True),
        name="gather_weights",
    )(*pieces)


def fits(mesh_shape, share):
    return mesh_shape["fsdp"] == 8 and mesh_shape["rep"] == 4 and share % 8 == 0


def gather(mesh_shape, pieces):
    if fits(mesh_shape, pieces[1].shape[0]):
        return gather_remote(mesh_shape, pieces)
    return gather_native(pieces)


def reduce_parts(depth, strips, terms, outs, scratch):
    count = len(terms)
    mine, theirs, relayed, direct, partial, below, above = (scratch[i * count : (i + 1) * count] for i in range(7))
    sems = scratch[7 * count :]
    (own_sem, core_sem, relay_sem, direct_sem, partial_sem, up_sem, down_sem) = sems[:7]
    (got_core, got_relay, got_direct, got_partial, got_below, got_above) = sems[7:]
    f, z, across_core, step_x, step_y = neighbours()

    def toward(n):
        return (step_x, step_y) if strips[n][3] else (step_y, step_x)

    def steps(n):
        first, second = toward(n)
        return (0, first, second, first + second)

    def term(n, who, plane):
        return cut(terms[strips[n][0]].at[who * depth + plane], strips[n])

    def cell(family, n, *index):
        return cut(family[strips[n][0]].at[index], strips[n])

    def own_copy(n, kind, plane):
        return pltpu.make_async_copy(term(n, f + steps(n)[kind], plane), cell(mine, n, kind, plane), own_sem.at[n, kind, plane])

    def core_copy(n, kind, plane):
        return remote(
            term(n, across_core + steps(n)[kind], plane),
            cell(theirs, n, kind, plane),
            core_sem.at[n, kind, plane],
            got_core.at[n, kind, plane],
            (across_core, z),
        )

    def relay(n, plane):
        return remote(cell(theirs, n, 3, plane), cell(relayed, n, plane), relay_sem.at[n, plane], got_relay.at[n, plane], (f + toward(n)[1], z))

    def straight(n, plane):
        return remote(cell(theirs, n, 2, plane), cell(direct, n, plane), direct_sem.at[n, plane], got_direct.at[n, plane], (f + toward(n)[1], z))

    def second_hop(n, plane):
        return remote(cell(theirs, n, 1, plane), cell(partial, n, plane), partial_sem.at[n, plane], got_partial.at[n, plane], (f + toward(n)[0], z))

    def go_up(n, plane):
        return remote(cell(theirs, n, 0, plane), cell(below, n, plane), up_sem.at[n, plane], got_below.at[n, plane], (f, z + 1))

    def go_down(n, plane):
        return remote(cell(theirs, n, 0, plane), cell(above, n, plane), down_sem.at[n, plane], got_above.at[n, plane], (f, z - 1))

    def add(n, kind, plane, *others):
        here = cell(theirs, n, kind, plane)
        total = here[...].astype(F32)
        for other in others:
            total = total + other[...].astype(F32)
        here[...] = total.astype(here.dtype)

    each = range(len(strips))
    order = (3, 2, 1, 0)

    def launch(t, carry):
        plane = far_first(t, z)
        for kind in order:
            for n in each:
                core_copy(n, kind, plane).start()
                own_copy(n, kind, plane).start()
        return carry

    def begin():
        meet(depth, f, z, across_core, step_x, step_y)
        lax.fori_loop(0, depth, launch, 0)

    def phase(t):
        plane = far_first(t, z)
        before = far_first(t - 1, z)
        earlier = far_first(t - 2, z)

        @pl.when(t < depth)
        def _():
            for kind in order:
                for n in each:
                    core_copy(n, kind, plane).wait_recv()
                    own_copy(n, kind, plane).wait()
                    add(n, kind, plane, cell(mine, n, kind, plane))
                if kind == 3:
                    for n in each:
                        relay(n, plane).start()
                if kind == 2:
                    for n in each:
                        straight(n, plane).start()

        @pl.when((t >= 1) & (t < depth + 1))
        def _():
            for n in each:
                relay(n, before).wait_recv()
                add(n, 1, before, cell(relayed, n, before))
            for n in each:
                second_hop(n, before).start()

        @pl.when(t >= 2)
        def _():
            for n in each:
                straight(n, earlier).wait_recv()
                second_hop(n, earlier).wait_recv()
                add(n, 0, earlier, cell(direct, n, earlier), cell(partial, n, earlier))

            @pl.when((earlier >= z) & (z > 0))
            def _():
                for n in each:
                    go_up(n, earlier).wait_recv()
                    add(n, 0, earlier, cell(below, n, earlier))

            @pl.when((earlier <= z) & (z < depth - 1))
            def _():
                for n in each:
                    go_down(n, earlier).wait_recv()
                    add(n, 0, earlier, cell(above, n, earlier))

            @pl.when(earlier > z)
            def _():
                for n in each:
                    go_up(n, earlier).start()

            @pl.when(earlier < z)
            def _():
                for n in each:
                    go_down(n, earlier).start()

    def close_plane(plane, carry):
        for n in each:
            for kind in order:
                core_copy(n, kind, plane).wait_send()
            relay(n, plane).wait_send()
            straight(n, plane).wait_send()
            second_hop(n, plane).wait_send()

        @pl.when(plane > z)
        def _():
            for n in each:
                go_up(n, plane).wait_send()

        @pl.when(plane < z)
        def _():
            for n in each:
                go_down(n, plane).wait_send()

        return carry

    def finish():
        for a in range(count):
            outs[a][...] = theirs[a][0, z].astype(F32)
        lax.fori_loop(0, depth, close_plane, 0)

    return begin, phase, finish


def reduce_kernel(depth, strips, count, *refs):
    terms, outs, scratch = refs[:count], refs[count : 2 * count], refs[2 * count :]
    begin, phase, finish = reduce_parts(depth, strips, terms, outs, scratch)
    begin()

    def step(t, carry):
        phase(t)
        return carry

    lax.fori_loop(0, depth + 2, step, 0)
    finish()


def reduce_scratch(terms, strips, depth):
    dma = pltpu.SemaphoreType.DMA
    flat, cored = dma((len(strips), depth)), dma((len(strips), 4, depth))
    whole = [pltpu.VMEM((4, depth) + t.shape[1:], t.dtype) for t in terms]
    line = [pltpu.VMEM((depth,) + t.shape[1:], t.dtype) for t in terms]
    return whole + whole + line * 5 + [cored, cored, flat, flat, flat, flat, flat, cored, flat, flat, flat, flat, flat]


def reduce_remote(mesh_shape, terms, collective_id=2):
    depth = mesh_shape["rep"]
    strips = strips_of([t.shape[1:] for t in terms])
    count = len(terms)
    return pl.pallas_call(
        functools.partial(reduce_kernel, depth, strips, count),
        out_shape=[jax.ShapeDtypeStruct(t.shape[1:], F32) for t in terms],
        in_specs=[pl.BlockSpec(memory_space=pl.ANY)] * count,
        out_specs=[pl.BlockSpec(memory_space=pltpu.VMEM)] * count,
        scratch_shapes=reduce_scratch(terms, strips, depth),
        compiler_params=pltpu.CompilerParams(
            collective_id=collective_id, has_side_effects=True, vmem_limit_bytes=48 * 1024 * 1024
        ),
        name="reduce_terms",
    )(*terms)


def reduce(mesh_shape, terms):
    if fits(mesh_shape, terms[1].shape[1]):
        return reduce_remote(mesh_shape, [t.astype(F32 if i == 0 else BF) for i, t in enumerate(terms)])
    return reduce_native(terms)


def lane_block(index, size):
    return pl.ds(pl.multiple_of(index * size, size), size)


def forward_kernel(depth, strips, count, heads_at_once, len_ref, x_ref, w_ref, b_ref, *refs):
    ins, refs = refs[:count], refs[count:]
    qkv_ref, ctx_ref, lse_ref = refs[:3]
    outs, sems = refs[3 : 3 + count], refs[3 + count :]
    begin, phase, finish = gather_parts(depth, strips, ins, outs, sems)
    width = x_ref.shape[1]
    seqs = len_ref.shape[0]
    length = x_ref.shape[0] // seqs
    block = heads_at_once * PAIR
    begin()

    def step(t, carry):
        j = t // 2

        @pl.when(t % 2 == 0)
        def _():
            for part in range(3):
                columns = pl.ds(pl.multiple_of(part * width + j * block, block), block)
                qkv_ref[:, columns] = (nn(x_ref[...], w_ref[:, columns]) + b_ref[:, columns]).astype(BF)

        @pl.when(t % 2 == 1)
        def _():
            def attend(i, inner):
                s, p = i // heads_at_once, j * heads_at_once + i % heads_at_once
                rows = lane_block(s, length)
                q2, k2, v2 = (
                    qkv_ref[rows, pl.ds(pl.multiple_of(part * width + p * PAIR, PAIR), PAIR)] for part in range(3)
                )
                ctx, low, high = forward_pair(len_ref[s], q2, k2, v2)
                ctx_ref[rows, lane_block(p, PAIR)] = ctx
                lse_ref[s, p, 0:1, :] = low
                lse_ref[s, p, 1:2, :] = high
                return inner

            lax.fori_loop(0, seqs * heads_at_once, attend, 0)

        @pl.when(t >= 1)
        def _():
            phase(t)

        return carry

    lax.fori_loop(0, depth + 2, step, 0)
    finish()


def forward_and_gather(mesh_shape, lengths, inputs, w_qkv, b_qkv, pieces, collective_id=3):
    depth, devices = mesh_shape["rep"], mesh_shape["rep"] * mesh_shape["fsdp"]
    strips = strips_of([p.shape for p in pieces])
    count = len(pieces)
    rows, width = inputs.shape
    seqs = lengths.shape[0]
    pairs = width // PAIR
    vmem = pl.BlockSpec(memory_space=pltpu.VMEM)
    out = pl.pallas_call(
        functools.partial(forward_kernel, depth, strips, count, pairs * 2 // (depth + 2)),
        out_shape=[
            jax.ShapeDtypeStruct((rows, 3 * width), BF),
            jax.ShapeDtypeStruct((rows, width), BF),
            jax.ShapeDtypeStruct((seqs, pairs, 2, rows // seqs), F32),
        ]
        + [jax.ShapeDtypeStruct((devices,) + p.shape, p.dtype) for p in pieces],
        in_specs=[pl.BlockSpec(memory_space=pltpu.SMEM)] + [vmem] * (3 + count),
        out_specs=[vmem] * 3 + [pl.BlockSpec(memory_space=pl.ANY)] * count,
        scratch_shapes=gather_semaphores(strips, count, depth),
        compiler_params=pltpu.CompilerParams(
            collective_id=collective_id, has_side_effects=True, vmem_limit_bytes=48 * 1024 * 1024
        ),
        name="forward_and_gather",
    )(lengths, inputs, w_qkv, b_qkv.reshape(1, 3 * width), *pieces)
    return out[0], out[1], out[2], out[3:]


def backward_kernel(depth, strips, count, heads_at_once, len_ref, x_ref, w_ref, qkv_ref, g_ref, ctx_ref, lse_ref, sum_ref, *refs):
    terms, refs = refs[:count], refs[count:]
    dw_ref, dx_ref, bias_ref = refs[:3]
    outs, refs = refs[3 : 3 + count], refs[3 + count :]
    dqkv_ref, total_ref, scratch = refs[0], refs[1], refs[2:]
    begin, phase, finish = reduce_parts(depth, strips, terms, outs, scratch)
    width = x_ref.shape[1]
    seqs = len_ref.shape[0]
    length = x_ref.shape[0] // seqs
    block = heads_at_once * PAIR
    begin()
    total_ref[...] = sum_ref[...]

    def step(t, carry):
        j = t // 2

        @pl.when(t % 2 == 0)
        def _():
            def attend(i, inner):
                s, p = i // heads_at_once, j * heads_at_once + i % heads_at_once
                rows = lane_block(s, length)
                places = [pl.ds(pl.multiple_of(part * width + p * PAIR, PAIR), PAIR) for part in range(3)]
                own = lane_block(p, PAIR)
                q2, k2, v2 = (qkv_ref[rows, place] for place in places)
                lses = [lse_ref[s, p, h : h + 1, :] for h in (0, 1)]
                grads = backward_pair(len_ref[s], q2, k2, v2, g_ref[rows, own], ctx_ref[rows, own], lses)
                for place, grad in zip(places, grads):
                    dqkv_ref[rows, place] = grad
                return inner

            lax.fori_loop(0, seqs * heads_at_once, attend, 0)

        @pl.when(t % 2 == 1)
        def _():
            for part in range(3):
                columns = pl.ds(pl.multiple_of(part * width + j * block, block), block)
                grad = dqkv_ref[:, columns]
                dw_ref[:, columns] = tn(x_ref[...], grad).astype(BF)
                bias_ref[:, columns] = jnp.sum(grad.astype(F32), axis=0, keepdims=True)
                total_ref[...] += nt(grad, w_ref[:, columns])

        phase(t)
        return carry

    lax.fori_loop(0, depth + 2, step, 0)
    dx_ref[...] = total_ref[...].astype(BF)
    finish()


def backward_and_reduce(mesh_shape, lengths, inputs, w_qkv, qkv, grad, ctx, lse, grad_sum, terms, collective_id=4):
    depth = mesh_shape["rep"]
    strips = strips_of([t.shape[1:] for t in terms])
    count = len(terms)
    rows, width = inputs.shape
    pairs = width // PAIR
    vmem = pl.BlockSpec(memory_space=pltpu.VMEM)
    out = pl.pallas_call(
        functools.partial(backward_kernel, depth, strips, count, pairs * 2 // (depth + 2)),
        out_shape=[
            jax.ShapeDtypeStruct((width, 3 * width), BF),
            jax.ShapeDtypeStruct((rows, width), BF),
            jax.ShapeDtypeStruct((1, 3 * width), F32),
        ]
        + [jax.ShapeDtypeStruct(t.shape[1:], F32) for t in terms],
        in_specs=[pl.BlockSpec(memory_space=pltpu.SMEM)] + [vmem] * 7 + [pl.BlockSpec(memory_space=pl.ANY)] * count,
        out_specs=[vmem] * (3 + count),
        scratch_shapes=[pltpu.VMEM((rows, 3 * width), BF), pltpu.VMEM((rows, width), F32)] + reduce_scratch(terms, strips, depth),
        compiler_params=pltpu.CompilerParams(
            collective_id=collective_id, has_side_effects=True, vmem_limit_bytes=63 * 1024 * 1024
        ),
        name="backward_and_reduce",
    )(lengths, inputs, w_qkv, qkv, grad, ctx, lse, grad_sum, *terms)
    return out[0], out[1], out[2], out[3:]

EPS = 1e-06
AXES = ("fsdp", "rep")


def norm_forward(hidden, gain, shift):
    mean = jnp.mean(hidden, axis=-1, keepdims=True)
    centred = hidden - mean
    inverse = lax.rsqrt(jnp.mean(centred * centred, axis=-1, keepdims=True) + EPS)
    normed = centred * inverse
    return (normed * gain + shift, normed, inverse)


def norm_backward(grad_out, normed, inverse, gain):
    grad_normed = grad_out * gain
    grad_in = inverse * (
        grad_normed
        - jnp.mean(grad_normed, axis=-1, keepdims=True)
        - normed * jnp.mean(grad_normed * normed, axis=-1, keepdims=True)
    )
    return (grad_in, jnp.sum(grad_out * normed, axis=0), jnp.sum(grad_out, axis=0))


def column_sums(grad):
    return jnp.sum(grad.astype(F32), axis=0)


def gather_native(pieces):
    return [lax.all_gather(p, AXES, axis=0, tiled=False) for p in pieces]


def reduce_native(terms):
    return [lax.psum_scatter(t.astype(F32), AXES, scatter_dimension=0, tiled=False) for t in terms]


def local(
    mesh_shape,
    hidden_in,
    lengths,
    query_weight,
    key_weight,
    value_weight,
    out_weight,
    up_weight,
    down_weight,
    query_bias,
    value_bias,
    out_bias,
    up_bias,
    down_bias,
    first_gain,
    first_shift,
    second_gain,
    second_shift,
    cotangent,
):
    seqs, length, width = hidden_in.shape
    rows = seqs * length
    hidden = up_weight.shape[1]
    share = query_weight.shape[0]
    spread = hidden // width
    devices = width // share
    vectors = jnp.concatenate(
        [
            jnp.stack([query_bias, value_bias, out_bias, down_bias, first_gain, first_shift, second_gain, second_shift]),
            up_bias.reshape(spread, share),
        ]
    )
    count = vectors.shape[0]
    vector_slot = jnp.pad(vectors, ((0, -count % 16), (0, -share % 128)))
    qkv_shard = jnp.concatenate([query_weight, key_weight, value_weight], axis=1)
    later = [out_weight, up_weight, down_weight]
    fused = fits(mesh_shape, share)
    got = gather(mesh_shape, [vector_slot, qkv_shard])
    w_qkv = got[1].reshape(width, 3 * width)
    wide = got[0].astype(F32)
    plain = jnp.transpose(wide[:, :8, :share], (1, 0, 2)).reshape(8, width)
    b_query, b_values, b_out, b_down, gain_one, shift_one, gain_two, shift_two = [plain[i] for i in range(8)]
    b_up = wide[:, 8 : 8 + spread, :share].reshape(hidden)

    inputs = hidden_in.reshape(rows, width)
    b_qkv = jnp.concatenate([b_query, jnp.zeros_like(b_query), b_values])
    if fused:
        qkv, context, log_sums, got = forward_and_gather(mesh_shape, lengths, inputs, w_qkv, b_qkv, later)
    else:
        got = gather(mesh_shape, later)
        qkv = (nn(inputs, w_qkv) + b_qkv).astype(BF)
        context, log_sums = attention_forward(lengths, qkv, seqs, length, width)
    w_out = got[0].reshape(width, width)
    w_up = got[1].reshape(width, hidden)
    w_down = got[2].reshape(hidden, width)
    first_sum = inputs.astype(F32) + nn(context, w_out) + b_out
    first, normed_one, inverse_one = norm_forward(first_sum, gain_one, shift_one)
    first_low = first.astype(BF)
    inner = nn(first_low, w_up) + b_up
    half = 0.5 * (1.0 + lax.erf(inner * (2.0**-0.5)))
    active = (inner * half).astype(BF)
    slope = half + inner * ((2.0 * math.pi) ** -0.5) * jnp.exp(-0.5 * inner * inner)
    slope = slope.astype(BF)
    second_sum = first + nn(active, w_down) + b_down
    result, normed_two, inverse_two = norm_forward(second_sum, gain_two, shift_two)
    hidden_out = result.astype(BF).reshape(seqs, length, width)
    grad_out = cotangent.reshape(rows, width).astype(F32)
    grad_second, grad_gain_two, grad_shift_two = norm_backward(grad_out, normed_two, inverse_two, gain_two)
    grad_branch = grad_second.astype(BF)
    grad_b_down = column_sums(grad_branch)
    grad_w_down = tn(active, grad_branch)
    grad_active = nt(grad_branch, w_down)
    grad_inner = (grad_active * slope.astype(F32)).astype(BF)
    grad_b_up = column_sums(grad_inner)
    grad_w_up = tn(first_low, grad_inner)
    grad_first = grad_second + nt(grad_inner, w_up)
    grad_first_sum, grad_gain_one, grad_shift_one = norm_backward(grad_first, normed_one, inverse_one, gain_one)
    grad_attn = grad_first_sum.astype(BF)
    grad_b_out = column_sums(grad_attn)
    grad_w_out = tn(context, grad_attn)
    grad_context = nt(grad_attn, w_out).astype(BF)
    later = [
        grad_w_out.reshape(devices, share, width),
        grad_w_up.reshape(devices, share, hidden),
        grad_w_down.reshape(devices, spread * share, width),
    ]
    if fused:
        later = [t.astype(BF) for t in later]
        grad_w_qkv, input_grad, bias_sums, owned_later = backward_and_reduce(
            mesh_shape, lengths, inputs, w_qkv, qkv, grad_context, context, log_sums, grad_first_sum, later
        )
        bias_sums = bias_sums[0]
    else:
        grad_query, grad_keys, grad_values = attention_backward(
            lengths, qkv, grad_context, context, log_sums, seqs, length, width
        )
        grad_qkv = jnp.concatenate([grad_query, grad_keys, grad_values], axis=1)
        input_grad = (grad_first_sum + nt(grad_qkv, w_qkv)).astype(BF)
        grad_w_qkv = tn(inputs, grad_qkv)
        bias_sums = column_sums(grad_qkv)
        owned_later = reduce_native(later)
    input_grad = input_grad.reshape(seqs, length, width)
    sums = jnp.stack(
        [
            bias_sums[:width],
            bias_sums[2 * width :],
            grad_b_out,
            grad_b_down,
            grad_gain_one,
            grad_shift_one,
            grad_gain_two,
            grad_shift_two,
        ]
    )
    vector_terms = jnp.concatenate(
        [jnp.transpose(sums.reshape(8, devices, share), (1, 0, 2)), grad_b_up.reshape(devices, spread, share)], axis=1
    )
    vector_terms = jnp.pad(vector_terms, ((0, 0), (0, -count % 16), (0, -share % 128)))
    owned = reduce(mesh_shape, [vector_terms, grad_w_qkv.reshape(devices, share, 3 * width)])
    vec = owned[0][:count, :share]
    return (
        hidden_out,
        input_grad,
        owned[1][:, :width],
        owned[1][:, width : 2 * width],
        owned[1][:, 2 * width :],
        owned_later[0],
        owned_later[1],
        owned_later[2],
        vec[0],
        vec[1],
        vec[2],
        vec[8:].reshape(spread * share),
        vec[3],
        vec[4],
        vec[5],
        vec[6],
        vec[7],
    )


def solution(mesh):
    rows = P(AXES, None)
    flat = P(AXES)
    cube = P(AXES, None, None)
    in_specs = (cube, flat) + (rows,) * 6 + (flat,) * 9 + (cube,)
    out_specs = (cube, cube) + (rows,) * 6 + (flat,) * 9
    body = functools.partial(local, dict(mesh.shape))
    return jax.shard_map(body, mesh=mesh, in_specs=in_specs, out_specs=out_specs, check_vma=False)
```

```python
import functools
import math

import jax
import jax.numpy as jnp
from jax import lax
from jax.experimental import pallas as pl
from jax.experimental.pallas import tpu as pltpu
from jax.sharding import PartitionSpec as P

HD = 64
PAIR = 2 * HD
BF = jnp.bfloat16
F32 = jnp.float32


def nt(left, right):
    return lax.dot_general(left, right, (((1,), (1,)), ((), ())), preferred_element_type=F32)


def nn(left, right):
    return jnp.dot(left, right, preferred_element_type=F32)


def tn(left, right):
    return lax.dot_general(left, right, (((0,), (0,)), ((), ())), preferred_element_type=F32)


def head_masks(length):
    lane = lax.broadcasted_iota(jnp.int32, (length, PAIR), 1)
    return lane


def masked_keys(k2, lane, head, valid):
    inside = (lane // HD) == head
    slot = lane == (1 - head) * HD
    row = lax.broadcasted_iota(jnp.int32, lane.shape, 0)
    bias = jnp.where(row < valid, 0.0, -1e30).astype(BF)
    return jnp.where(inside, k2, jnp.where(slot, bias, jnp.zeros_like(k2)))


def masked_query(q2, lane, head):
    inside = (lane // HD) == head
    slot = lane == (1 - head) * HD
    return jnp.where(inside, q2, jnp.where(slot, jnp.ones_like(q2), jnp.zeros_like(q2)))


def forward_pair(valid, q2, k2, v2):
    lane = head_masks(q2.shape[0])
    first = lane < HD
    q2 = q2 * BF(0.125)
    outs, tops = [], []
    for h in (0, 1):
        s = nt(masked_query(q2, lane, h), masked_keys(k2, lane, h, valid))
        top = jnp.max(s, axis=1, keepdims=True)
        e = jnp.exp(s - top).astype(BF)
        outs.append(nn(e, jnp.where((lane // HD) == h, v2, jnp.ones_like(v2))))
        tops.append(top)
    num = jnp.where(first, outs[0], outs[1])
    den = pltpu.roll(jnp.where(first, outs[1], outs[0]), HD, 1)
    lse = jnp.where(first, tops[0], tops[1]) + jnp.log(den)
    turned = lse.T
    return (num / den).astype(BF), turned[0:1], turned[HD : HD + 1]


def attention_forward_kernel(len_ref, q_ref, k_ref, v_ref, ctx_ref, lse_ref):
    ctx, low, high = forward_pair(len_ref[pl.program_id(0)], q_ref[...], k_ref[...], v_ref[...])
    ctx_ref[...] = ctx
    lse_ref[0, 0, 0:1, :] = low
    lse_ref[0, 0, 1:2, :] = high


def attention_forward(lengths, qkv, seqs, length, width):
    pairs = width // PAIR
    return pl.pallas_call(
        attention_forward_kernel,
        grid_spec=pltpu.PrefetchScalarGridSpec(
            num_scalar_prefetch=1,
            grid=(seqs, pairs),
            in_specs=[
                pl.BlockSpec((length, PAIR), lambda s, p, n: (s, p)),
                pl.BlockSpec((length, PAIR), lambda s, p, n: (s, pairs + p)),
                pl.BlockSpec((length, PAIR), lambda s, p, n: (s, 2 * pairs + p)),
            ],
            out_specs=[
                pl.BlockSpec((length, PAIR), lambda s, p, n: (s, p)),
                pl.BlockSpec((1, 1, 2, length), lambda s, p, n: (s, p, 0, 0)),
            ],
        ),
        out_shape=[
            jax.ShapeDtypeStruct((seqs * length, width), BF),
            jax.ShapeDtypeStruct((seqs, pairs, 2, length), F32),
        ],
        name="attention_forward",
    )(lengths, qkv, qkv, qkv)


def backward_pair(valid, q2, k2, v2, g2, ctx2, lses):
    lane = head_masks(q2.shape[0])
    first = lane < HD
    q2 = q2 * BF(0.125)
    k8 = k2 * BF(0.125)
    turned = (g2.astype(F32) * ctx2.astype(F32)).T
    dqs, dks, dvs = [], [], []
    for h in (0, 1):
        km = masked_keys(k2, lane, h, valid)
        qm = masked_query(q2, lane, h)
        vm = jnp.where((lane // HD) == h, v2, jnp.zeros_like(v2))
        delta = jnp.sum(turned[h * HD : (h + 1) * HD], axis=0, keepdims=True)
        p = jnp.exp(nt(km, qm) - lses[h])
        ds = (p * (nt(vm, g2) - delta)).astype(BF)
        dvs.append(nn(p.astype(BF), g2))
        dks.append(nn(ds, q2))
        dqs.append(tn(ds, k8))
    return [jnp.where(first, pair[0], pair[1]).astype(BF) for pair in (dqs, dks, dvs)]


def attention_backward_kernel(len_ref, q_ref, k_ref, v_ref, g_ref, ctx_ref, lse_ref, dq_ref, dk_ref, dv_ref):
    lses = [lse_ref[0, 0, h : h + 1, :] for h in (0, 1)]
    valid = len_ref[pl.program_id(0)]
    dq_ref[...], dk_ref[...], dv_ref[...] = backward_pair(
        valid, q_ref[...], k_ref[...], v_ref[...], g_ref[...], ctx_ref[...], lses
    )


def attention_backward(lengths, qkv, grad, ctx, lse, seqs, length, width):
    pairs = width // PAIR
    col = lambda k: pl.BlockSpec((length, PAIR), lambda s, p, n: (s, k * pairs + p))
    return pl.pallas_call(
        attention_backward_kernel,
        grid_spec=pltpu.PrefetchScalarGridSpec(
            num_scalar_prefetch=1,
            grid=(seqs, pairs),
            in_specs=[col(0), col(1), col(2), col(0), col(0), pl.BlockSpec((1, 1, 2, length), lambda s, p, n: (s, p, 0, 0))],
            out_specs=[col(0), col(0), col(0)],
        ),
        out_shape=[jax.ShapeDtypeStruct((seqs * length, width), BF)] * 3,
        name="attention_backward",
    )(lengths, qkv, qkv, qkv, grad, ctx, lse)


def neighbours():
    f, z = lax.axis_index("fsdp"), lax.axis_index("rep")
    core, x, y = f % 2, (f // 2) % 2, f // 4
    across_core = f + 1 - 2 * core
    step_x, step_y = 2 * (1 - 2 * x), 4 * (1 - 2 * y)
    return f, z, across_core, step_x, step_y


def remote(src, dst, send_sem, recv_sem, device):
    return pltpu.make_async_remote_copy(
        src_ref=src,
        dst_ref=dst,
        send_sem=send_sem,
        recv_sem=recv_sem,
        device_id=device,
        device_id_type=pl.DeviceIdType.MESH,
    )


def meet(depth, f, z, across_core, step_x, step_y):
    barrier = pltpu.get_barrier_semaphore()

    def greet(device):
        pl.semaphore_signal(barrier, inc=1, device_id=device, device_id_type=pl.DeviceIdType.MESH)

    for other in (across_core, f + step_x, f + step_y):
        greet((other, z))

    @pl.when(z > 0)
    def _():
        greet((f, z - 1))

    @pl.when(z < depth - 1)
    def _():
        greet((f, z + 1))

    pl.semaphore_wait(barrier, 3 + jnp.minimum(z, 1) + jnp.minimum(depth - 1 - z, 1))


def far_first(step, z):
    zero = 3 * (1 - z // 2)
    one = (2 + 3 * z) % 5
    two = 1 + z % 2
    picks = (zero, one, two, z)
    total = 0
    for i, pick in enumerate(picks):
        hit = 1 - jnp.minimum(jnp.abs(step - i), 1)
        total = total + hit * pick
    return total


def strips_of(arrays):
    found = []
    for index, array in enumerate(arrays):
        columns = array[1]
        if columns % 256 == 0:
            found.append((index, 0, columns // 2, True))
            found.append((index, columns // 2, columns // 2, False))
        else:
            found.append((index, 0, None, True))
    return found


def cut(ref, strip):
    if strip[2] is None:
        return ref
    return ref.at[:, pl.ds(strip[1], strip[2])]


def gather_parts(depth, strips, ins, outs, sems):
    count = len(ins)
    (own_sem, up_sem, down_sem, first_sem, second_sem, relay_sem, core_sem) = sems[:7]
    (got_column, got_first, got_second, got_diagonal, got_core) = sems[7:]
    f, z, across_core, step_x, step_y = neighbours()

    def slot(who, plane):
        return who * depth + plane

    def place(n, who, plane):
        return cut(outs[strips[n][0]].at[slot(who, plane)], strips[n])

    def toward(n):
        return (step_x, step_y) if strips[n][3] else (step_y, step_x)

    def own_copy(a):
        return pltpu.make_async_copy(ins[a], outs[a].at[slot(f, z)], own_sem.at[a])

    def core_copy(n, kind, plane, src):
        first, second = toward(n)
        who = f + (0, first, second, first + second)[kind]
        where = place(n, who, plane)
        return remote(where if src is None else src, where, core_sem.at[n, kind, plane], got_core.at[n, kind, plane], (across_core, z))

    def core_arrival(n, kind, plane):
        first, second = toward(n)
        who = across_core + (0, first, second, first + second)[kind]
        where = place(n, who, plane)
        return remote(where, where, core_sem.at[n, kind, plane], got_core.at[n, kind, plane], (across_core, z))

    def column_up(n, plane, src):
        return remote(src, place(n, f, plane), up_sem.at[n, plane], got_column.at[n, plane], (f, z + 1))

    def column_down(n, plane, src):
        return remote(src, place(n, f, plane), down_sem.at[n, plane], got_column.at[n, plane], (f, z - 1))

    def to_first(n, plane, src):
        return remote(src, place(n, f, plane), first_sem.at[n, plane], got_first.at[n, plane], (f + toward(n)[0], z))

    def to_second(n, plane, src):
        return remote(src, place(n, f, plane), second_sem.at[n, plane], got_second.at[n, plane], (f + toward(n)[1], z))

    def relay(n, plane):
        where = place(n, f + toward(n)[0], plane)
        return remote(where, where, relay_sem.at[n, plane], got_diagonal.at[n, plane], (f + toward(n)[1], z))

    def each(body):
        for n in range(len(strips)):
            body(n)

    def send_own(n):
        src = cut(ins[strips[n][0]], strips[n])
        to_first(n, z, src).start()
        to_second(n, z, src).start()

        @pl.when(z < depth - 1)
        def _():
            column_up(n, z, src).start()

        @pl.when(z > 0)
        def _():
            column_down(n, z, src).start()

        core_copy(n, 0, z, src).start()

    def begin():
        meet(depth, f, z, across_core, step_x, step_y)
        for a in range(count):
            own_copy(a).start()
        each(send_own)

    def phase(t):
        plane = far_first(depth - 1 - t, z)
        before = far_first(depth - t, z)
        earlier = far_first(depth + 1 - t, z)

        @pl.when((t >= 1) & (t < depth))
        def _():
            def arrived(n):
                src = place(n, f, plane)
                remote(src, src, up_sem.at[n, plane], got_column.at[n, plane], (f, z)).wait_recv()
                to_first(n, plane, src).start()
                to_second(n, plane, src).start()

                @pl.when((plane < z) & (z < depth - 1))
                def _():
                    column_up(n, plane, src).start()

                @pl.when((plane > z) & (z > 0))
                def _():
                    column_down(n, plane, src).start()

                core_copy(n, 0, plane, None).start()

            each(arrived)

        @pl.when((t >= 1) & (t < depth + 1))
        def _():
            def beside(n):
                first, second = toward(n)
                here = place(n, f + first, before)
                remote(here, here, first_sem.at[n, before], got_first.at[n, before], (f + first, z)).wait_recv()
                relay(n, before).start()
                core_copy(n, 1, before, None).start()

            each(beside)

            def above(n):
                first, second = toward(n)
                here = place(n, f + second, before)
                remote(here, here, second_sem.at[n, before], got_second.at[n, before], (f + second, z)).wait_recv()
                core_copy(n, 2, before, None).start()

            each(above)

        @pl.when(t >= 2)
        def _():
            def opposite(n):
                first, second = toward(n)
                here = place(n, f + first + second, earlier)
                remote(here, here, relay_sem.at[n, earlier], got_diagonal.at[n, earlier], (f + second, z)).wait_recv()
                core_copy(n, 3, earlier, None).start()

            each(opposite)

    def close_plane(plane, carry):
        def close(n):
            src = place(n, f, plane)
            to_first(n, plane, src).wait_send()
            to_second(n, plane, src).wait_send()
            relay(n, plane).wait_send()

            @pl.when((plane <= z) & (z < depth - 1))
            def _():
                column_up(n, plane, src).wait_send()

            @pl.when((plane >= z) & (z > 0))
            def _():
                column_down(n, plane, src).wait_send()

            for kind in range(4):
                core_copy(n, kind, plane, None).wait_send()
                core_arrival(n, kind, plane).wait_recv()

        each(close)
        return carry

    def finish():
        for a in range(count):
            own_copy(a).wait()
        lax.fori_loop(0, depth, close_plane, 0)

    return begin, phase, finish


def gather_kernel(depth, strips, count, *refs):
    ins, outs, sems = refs[:count], refs[count : 2 * count], refs[2 * count :]
    begin, phase, finish = gather_parts(depth, strips, ins, outs, sems)
    begin()

    def step(t, carry):
        phase(t)
        return carry

    lax.fori_loop(1, depth + 2, step, 0)
    finish()


def gather_semaphores(strips, count, depth):
    dma = pltpu.SemaphoreType.DMA
    flat, cored = dma((len(strips), depth)), dma((len(strips), 4, depth))
    return [dma((count,)), flat, flat, flat, flat, flat, cored, flat, flat, flat, flat, cored]


def gather_remote(mesh_shape, pieces):
    depth, devices = mesh_shape["rep"], mesh_shape["rep"] * mesh_shape["fsdp"]
    strips = strips_of([p.shape for p in pieces])
    count = len(pieces)
    return pl.pallas_call(
        functools.partial(gather_kernel, depth, strips, count),
        out_shape=[jax.ShapeDtypeStruct((devices,) + p.shape, p.dtype) for p in pieces],
        in_specs=[pl.BlockSpec(memory_space=pltpu.VMEM)] * count,
        out_specs=[pl.BlockSpec(memory_space=pl.ANY)] * count,
        scratch_shapes=gather_semaphores(strips, count, depth),
        compiler_params=pltpu.CompilerParams(collective_id=1, has_side_effects=True),
        name="gather_weights",
    )(*pieces)


def fits(mesh_shape, share):
    return mesh_shape["fsdp"] == 8 and mesh_shape["rep"] == 4 and share % 8 == 0


def gather(mesh_shape, pieces):
    if fits(mesh_shape, pieces[1].shape[0]):
        return gather_remote(mesh_shape, pieces)
    return gather_native(pieces)


def reduce_parts(depth, strips, terms, outs, scratch):
    count = len(terms)
    mine, theirs, relayed, direct, partial, below, above = (scratch[i * count : (i + 1) * count] for i in range(7))
    sems = scratch[7 * count :]
    (own_sem, core_sem, relay_sem, direct_sem, partial_sem, up_sem, down_sem) = sems[:7]
    (got_core, got_relay, got_direct, got_partial, got_below, got_above) = sems[7:]
    f, z, across_core, step_x, step_y = neighbours()

    def toward(n):
        return (step_x, step_y) if strips[n][3] else (step_y, step_x)

    def steps(n):
        first, second = toward(n)
        return (0, first, second, first + second)

    def term(n, who, plane):
        return cut(terms[strips[n][0]].at[who * depth + plane], strips[n])

    def cell(family, n, *index):
        return cut(family[strips[n][0]].at[index], strips[n])

    def own_copy(n, kind, plane):
        return pltpu.make_async_copy(term(n, f + steps(n)[kind], plane), cell(mine, n, kind, plane), own_sem.at[n, kind, plane])

    def core_copy(n, kind, plane):
        return remote(
            term(n, across_core + steps(n)[kind], plane),
            cell(theirs, n, kind, plane),
            core_sem.at[n, kind, plane],
            got_core.at[n, kind, plane],
            (across_core, z),
        )

    def relay(n, plane):
        return remote(cell(theirs, n, 3, plane), cell(relayed, n, plane), relay_sem.at[n, plane], got_relay.at[n, plane], (f + toward(n)[1], z))

    def straight(n, plane):
        return remote(cell(theirs, n, 2, plane), cell(direct, n, plane), direct_sem.at[n, plane], got_direct.at[n, plane], (f + toward(n)[1], z))

    def second_hop(n, plane):
        return remote(cell(theirs, n, 1, plane), cell(partial, n, plane), partial_sem.at[n, plane], got_partial.at[n, plane], (f + toward(n)[0], z))

    def go_up(n, plane):
        return remote(cell(theirs, n, 0, plane), cell(below, n, plane), up_sem.at[n, plane], got_below.at[n, plane], (f, z + 1))

    def go_down(n, plane):
        return remote(cell(theirs, n, 0, plane), cell(above, n, plane), down_sem.at[n, plane], got_above.at[n, plane], (f, z - 1))

    def add(n, kind, plane, *others):
        here = cell(theirs, n, kind, plane)
        total = here[...].astype(F32)
        for other in others:
            total = total + other[...].astype(F32)
        here[...] = total.astype(here.dtype)

    each = range(len(strips))
    order = (3, 2, 1, 0)

    def launch(t, carry):
        plane = far_first(t, z)
        for kind in order:
            for n in each:
                core_copy(n, kind, plane).start()
                own_copy(n, kind, plane).start()
        return carry

    def begin():
        meet(depth, f, z, across_core, step_x, step_y)
        lax.fori_loop(0, depth, launch, 0)

    def phase(t):
        plane = far_first(t, z)
        before = far_first(t - 1, z)
        earlier = far_first(t - 2, z)

        @pl.when(t < depth)
        def _():
            for kind in order:
                for n in each:
                    core_copy(n, kind, plane).wait_recv()
                    own_copy(n, kind, plane).wait()
                    add(n, kind, plane, cell(mine, n, kind, plane))
                if kind == 3:
                    for n in each:
                        relay(n, plane).start()
                if kind == 2:
                    for n in each:
                        straight(n, plane).start()

        @pl.when((t >= 1) & (t < depth + 1))
        def _():
            for n in each:
                relay(n, before).wait_recv()
                add(n, 1, before, cell(relayed, n, before))
            for n in each:
                second_hop(n, before).start()

        @pl.when(t >= 2)
        def _():
            for n in each:
                straight(n, earlier).wait_recv()
                second_hop(n, earlier).wait_recv()
                add(n, 0, earlier, cell(direct, n, earlier), cell(partial, n, earlier))

            @pl.when((earlier >= z) & (z > 0))
            def _():
                for n in each:
                    go_up(n, earlier).wait_recv()
                    add(n, 0, earlier, cell(below, n, earlier))

            @pl.when((earlier <= z) & (z < depth - 1))
            def _():
                for n in each:
                    go_down(n, earlier).wait_recv()
                    add(n, 0, earlier, cell(above, n, earlier))

            @pl.when(earlier > z)
            def _():
                for n in each:
                    go_up(n, earlier).start()

            @pl.when(earlier < z)
            def _():
                for n in each:
                    go_down(n, earlier).start()

    def close_plane(plane, carry):
        for n in each:
            for kind in order:
                core_copy(n, kind, plane).wait_send()
            relay(n, plane).wait_send()
            straight(n, plane).wait_send()
            second_hop(n, plane).wait_send()

        @pl.when(plane > z)
        def _():
            for n in each:
                go_up(n, plane).wait_send()

        @pl.when(plane < z)
        def _():
            for n in each:
                go_down(n, plane).wait_send()

        return carry

    def finish():
        for a in range(count):
            outs[a][...] = theirs[a][0, z].astype(F32)
        lax.fori_loop(0, depth, close_plane, 0)

    return begin, phase, finish


def reduce_kernel(depth, strips, count, *refs):
    terms, outs, scratch = refs[:count], refs[count : 2 * count], refs[2 * count :]
    begin, phase, finish = reduce_parts(depth, strips, terms, outs, scratch)
    begin()

    def step(t, carry):
        phase(t)
        return carry

    lax.fori_loop(0, depth + 2, step, 0)
    finish()


def reduce_scratch(terms, strips, depth):
    dma = pltpu.SemaphoreType.DMA
    flat, cored = dma((len(strips), depth)), dma((len(strips), 4, depth))
    whole = [pltpu.VMEM((4, depth) + t.shape[1:], t.dtype) for t in terms]
    line = [pltpu.VMEM((depth,) + t.shape[1:], t.dtype) for t in terms]
    return whole + whole + line * 5 + [cored, cored, flat, flat, flat, flat, flat, cored, flat, flat, flat, flat, flat]


def reduce_remote(mesh_shape, terms, collective_id=2):
    depth = mesh_shape["rep"]
    strips = strips_of([t.shape[1:] for t in terms])
    count = len(terms)
    return pl.pallas_call(
        functools.partial(reduce_kernel, depth, strips, count),
        out_shape=[jax.ShapeDtypeStruct(t.shape[1:], F32) for t in terms],
        in_specs=[pl.BlockSpec(memory_space=pl.ANY)] * count,
        out_specs=[pl.BlockSpec(memory_space=pltpu.VMEM)] * count,
        scratch_shapes=reduce_scratch(terms, strips, depth),
        compiler_params=pltpu.CompilerParams(
            collective_id=collective_id, has_side_effects=True, vmem_limit_bytes=48 * 1024 * 1024
        ),
        name="reduce_terms",
    )(*terms)


def reduce(mesh_shape, terms):
    if fits(mesh_shape, terms[1].shape[1]):
        return reduce_remote(mesh_shape, [t.astype(F32 if i == 0 else BF) for i, t in enumerate(terms)])
    return reduce_native(terms)


def lane_block(index, size):
    return pl.ds(pl.multiple_of(index * size, size), size)


def forward_kernel(depth, strips, count, heads_at_once, len_ref, x_ref, w_ref, b_ref, *refs):
    ins, refs = refs[:count], refs[count:]
    qkv_ref, ctx_ref, lse_ref = refs[:3]
    outs, sems = refs[3 : 3 + count], refs[3 + count :]
    begin, phase, finish = gather_parts(depth, strips, ins, outs, sems)
    width = x_ref.shape[1]
    seqs = len_ref.shape[0]
    length = x_ref.shape[0] // seqs
    block = heads_at_once * PAIR
    begin()

    def step(t, carry):
        j = t // 2

        @pl.when(t % 2 == 0)
        def _():
            for part in range(3):
                columns = pl.ds(pl.multiple_of(part * width + j * block, block), block)
                qkv_ref[:, columns] = (nn(x_ref[...], w_ref[:, columns]) + b_ref[:, columns]).astype(BF)

        @pl.when(t % 2 == 1)
        def _():
            def attend(i, inner):
                s, p = i // heads_at_once, j * heads_at_once + i % heads_at_once
                rows = lane_block(s, length)
                q2, k2, v2 = (
                    qkv_ref[rows, pl.ds(pl.multiple_of(part * width + p * PAIR, PAIR), PAIR)] for part in range(3)
                )
                ctx, low, high = forward_pair(len_ref[s], q2, k2, v2)
                ctx_ref[rows, lane_block(p, PAIR)] = ctx
                lse_ref[s, p, 0:1, :] = low
                lse_ref[s, p, 1:2, :] = high
                return inner

            lax.fori_loop(0, seqs * heads_at_once, attend, 0)

        @pl.when(t >= 1)
        def _():
            phase(t)

        return carry

    lax.fori_loop(0, depth + 2, step, 0)
    finish()


def forward_and_gather(mesh_shape, lengths, inputs, w_qkv, b_qkv, pieces, collective_id=3):
    depth, devices = mesh_shape["rep"], mesh_shape["rep"] * mesh_shape["fsdp"]
    strips = strips_of([p.shape for p in pieces])
    count = len(pieces)
    rows, width = inputs.shape
    seqs = lengths.shape[0]
    pairs = width // PAIR
    vmem = pl.BlockSpec(memory_space=pltpu.VMEM)
    out = pl.pallas_call(
        functools.partial(forward_kernel, depth, strips, count, pairs * 2 // (depth + 2)),
        out_shape=[
            jax.ShapeDtypeStruct((rows, 3 * width), BF),
            jax.ShapeDtypeStruct((rows, width), BF),
            jax.ShapeDtypeStruct((seqs, pairs, 2, rows // seqs), F32),
        ]
        + [jax.ShapeDtypeStruct((devices,) + p.shape, p.dtype) for p in pieces],
        in_specs=[pl.BlockSpec(memory_space=pltpu.SMEM)] + [vmem] * (3 + count),
        out_specs=[vmem] * 3 + [pl.BlockSpec(memory_space=pl.ANY)] * count,
        scratch_shapes=gather_semaphores(strips, count, depth),
        compiler_params=pltpu.CompilerParams(
            collective_id=collective_id, has_side_effects=True, vmem_limit_bytes=48 * 1024 * 1024
        ),
        name="forward_and_gather",
    )(lengths, inputs, w_qkv, b_qkv.reshape(1, 3 * width), *pieces)
    return out[0], out[1], out[2], out[3:]


def backward_kernel(depth, strips, count, heads_at_once, len_ref, x_ref, w_ref, qkv_ref, g_ref, ctx_ref, lse_ref, sum_ref, *refs):
    terms, refs = refs[:count], refs[count:]
    dw_ref, dx_ref, bias_ref = refs[:3]
    outs, refs = refs[3 : 3 + count], refs[3 + count :]
    dqkv_ref, total_ref, scratch = refs[0], refs[1], refs[2:]
    begin, phase, finish = reduce_parts(depth, strips, terms, outs, scratch)
    width = x_ref.shape[1]
    seqs = len_ref.shape[0]
    length = x_ref.shape[0] // seqs
    block = heads_at_once * PAIR
    begin()
    total_ref[...] = sum_ref[...]

    def step(t, carry):
        j = t // 2

        @pl.when(t % 2 == 0)
        def _():
            def attend(i, inner):
                s, p = i // heads_at_once, j * heads_at_once + i % heads_at_once
                rows = lane_block(s, length)
                places = [pl.ds(pl.multiple_of(part * width + p * PAIR, PAIR), PAIR) for part in range(3)]
                own = lane_block(p, PAIR)
                q2, k2, v2 = (qkv_ref[rows, place] for place in places)
                lses = [lse_ref[s, p, h : h + 1, :] for h in (0, 1)]
                grads = backward_pair(len_ref[s], q2, k2, v2, g_ref[rows, own], ctx_ref[rows, own], lses)
                for place, grad in zip(places, grads):
                    dqkv_ref[rows, place] = grad
                return inner

            lax.fori_loop(0, seqs * heads_at_once, attend, 0)

        @pl.when(t % 2 == 1)
        def _():
            for part in range(3):
                columns = pl.ds(pl.multiple_of(part * width + j * block, block), block)
                grad = dqkv_ref[:, columns]
                dw_ref[:, columns] = tn(x_ref[...], grad).astype(BF)
                bias_ref[:, columns] = jnp.sum(grad.astype(F32), axis=0, keepdims=True)
                total_ref[...] += nt(grad, w_ref[:, columns])

        phase(t)
        return carry

    lax.fori_loop(0, depth + 2, step, 0)
    dx_ref[...] = total_ref[...].astype(BF)
    finish()


def backward_and_reduce(mesh_shape, lengths, inputs, w_qkv, qkv, grad, ctx, lse, grad_sum, terms, collective_id=4):
    depth = mesh_shape["rep"]
    strips = strips_of([t.shape[1:] for t in terms])
    count = len(terms)
    rows, width = inputs.shape
    pairs = width // PAIR
    vmem = pl.BlockSpec(memory_space=pltpu.VMEM)
    out = pl.pallas_call(
        functools.partial(backward_kernel, depth, strips, count, pairs * 2 // (depth + 2)),
        out_shape=[
            jax.ShapeDtypeStruct((width, 3 * width), BF),
            jax.ShapeDtypeStruct((rows, width), BF),
            jax.ShapeDtypeStruct((1, 3 * width), F32),
        ]
        + [jax.ShapeDtypeStruct(t.shape[1:], F32) for t in terms],
        in_specs=[pl.BlockSpec(memory_space=pltpu.SMEM)] + [vmem] * 7 + [pl.BlockSpec(memory_space=pl.ANY)] * count,
        out_specs=[vmem] * (3 + count),
        scratch_shapes=[pltpu.VMEM((rows, 3 * width), BF), pltpu.VMEM((rows, width), F32)] + reduce_scratch(terms, strips, depth),
        compiler_params=pltpu.CompilerParams(
            collective_id=collective_id, has_side_effects=True, vmem_limit_bytes=63 * 1024 * 1024
        ),
        name="backward_and_reduce",
    )(lengths, inputs, w_qkv, qkv, grad, ctx, lse, grad_sum, *terms)
    return out[0], out[1], out[2], out[3:]


def norm_stats(hidden):
    mean = jnp.mean(hidden, axis=-1, keepdims=True)
    centred = hidden - mean
    inverse = lax.rsqrt(jnp.mean(centred * centred, axis=-1, keepdims=True) + EPS)
    return centred * inverse, inverse


def norm_pull(grad_normed, normed, inverse):
    return inverse * (
        grad_normed
        - jnp.mean(grad_normed, axis=-1, keepdims=True)
        - normed * jnp.mean(grad_normed * normed, axis=-1, keepdims=True)
    )


def total_rows(value):
    return jnp.sum(value.astype(F32), axis=0, keepdims=True)


def middle_kernel(depth, strips, x_ref, ctx_ref, cot_ref, w_out_ref, w_up_ref, w_down_ref, vec_ref, b_up_ref, *refs):
    hidden_ref, sum_ref, grad_ctx_ref, dw_out_ref, dw_up_ref, vec_out_ref, b_up_out_ref, owned_ref = refs[:8]
    active_ref, slope_ref, low_ref, normed_ref, inverse_ref, branch_ref, terms_ref = refs[8:15]
    begin, phase, finish = reduce_parts(depth, strips, (terms_ref,), (owned_ref,), refs[15:])
    rows, width = x_ref.shape
    hidden = w_up_ref.shape[1]
    chunk, block = 256, 256

    def vector(i):
        return vec_ref[i : i + 1, :]

    def put(i, value):
        vec_out_ref[i : i + 1, :] += value

    vec_out_ref[...] = jnp.zeros_like(vec_out_ref)

    def attention_out(i, carry):
        part = lane_block(i, chunk)
        first_sum = x_ref[part, :].astype(F32) + nn(ctx_ref[part, :], w_out_ref[...]) + vector(2)
        normed, inverse = norm_stats(first_sum)
        first = normed * vector(4) + vector(5)
        normed_ref[part, :] = normed
        inverse_ref[part, :] = inverse
        sum_ref[part, :] = first
        low_ref[part, :] = first.astype(BF)
        return carry

    lax.fori_loop(0, rows // chunk, attention_out, 0)

    def up(j, carry):
        columns = lane_block(j, block)
        inner = nn(low_ref[...], w_up_ref[:, columns]) + b_up_ref[:, columns]
        half = 0.5 + 0.5 * lax.erf(inner * (2.0**-0.5))
        active_ref[:, columns] = (inner * half).astype(BF)
        slope_ref[:, columns] = (half + inner * ((2.0 * math.pi) ** -0.5) * jnp.exp(-0.5 * inner * inner)).astype(BF)
        return carry

    lax.fori_loop(0, hidden // block, up, 0)

    def down(i, carry):
        part = lane_block(i, chunk)
        second_sum = sum_ref[part, :] + nn(active_ref[part, :], w_down_ref[...]) + vector(3)
        normed, inverse = norm_stats(second_sum)
        hidden_ref[part, :] = (normed * vector(6) + vector(7)).astype(BF)
        grad_out = cot_ref[part, :].astype(F32)
        put(6, total_rows(grad_out * normed))
        put(7, total_rows(grad_out))
        grad_second = norm_pull(grad_out * vector(6), normed, inverse)
        sum_ref[part, :] = grad_second
        branch = grad_second.astype(BF)
        branch_ref[part, :] = branch
        put(3, total_rows(branch))
        return carry

    lax.fori_loop(0, rows // chunk, down, 0)

    share = terms_ref.shape[1]
    slots = 4

    def down_terms(i, carry):
        term = tn(active_ref[:, lane_block(i, slots * share)], branch_ref[...])
        terms_ref[pl.ds(i * slots, slots)] = term.astype(BF).reshape(slots, share, width)
        return carry

    lax.fori_loop(0, terms_ref.shape[0] // slots, down_terms, 0)
    begin()
    blocks = hidden // block
    stride = blocks // depth

    def up_back(j, carry):
        columns = lane_block(j, block)
        grad_active = nt(branch_ref[...], w_down_ref[columns, :])
        grad_inner = (grad_active * slope_ref[:, columns].astype(F32)).astype(BF)
        slope_ref[:, columns] = grad_inner
        b_up_out_ref[:, columns] = total_rows(grad_inner)
        dw_up_ref[:, columns] = tn(low_ref[...], grad_inner).astype(BF)

        @pl.when(j % stride == stride - 1)
        def _():
            phase(j // stride)

        return carry

    lax.fori_loop(0, blocks, up_back, 0)

    def first_back(i, carry):
        part = lane_block(i, chunk)
        grad_first = sum_ref[part, :] + nt(slope_ref[part, :], w_up_ref[...])
        normed = normed_ref[part, :]
        put(4, total_rows(grad_first * normed))
        put(5, total_rows(grad_first))
        grad = norm_pull(grad_first * vector(4), normed, inverse_ref[part, :])
        sum_ref[part, :] = grad
        low = grad.astype(BF)
        branch_ref[part, :] = low
        put(2, total_rows(low))
        grad_ctx_ref[part, :] = nt(low, w_out_ref[...]).astype(BF)
        return carry

    lax.fori_loop(0, rows // chunk, first_back, 0)
    dw_out_ref[...] = tn(ctx_ref[...], branch_ref[...]).astype(BF)
    lax.fori_loop(depth, depth + 2, lambda t, carry: (phase(t), carry)[1], 0)
    finish()


def middle(mesh_shape, inputs, context, cotangent, w_out, w_up, w_down, plain, b_up, collective_id=5):
    depth, devices = mesh_shape["rep"], mesh_shape["rep"] * mesh_shape["fsdp"]
    rows, width = inputs.shape
    hidden = w_up.shape[1]
    terms = jax.ShapeDtypeStruct((devices, hidden // devices, width), BF)
    strips = strips_of([terms.shape[1:]])
    vmem = pl.BlockSpec(memory_space=pltpu.VMEM)
    shape = jax.ShapeDtypeStruct
    return pl.pallas_call(
        functools.partial(middle_kernel, depth, strips),
        out_shape=[
            shape((rows, width), BF),
            shape((rows, width), F32),
            shape((rows, width), BF),
            shape((width, width), BF),
            shape((width, hidden), BF),
            shape((8, width), F32),
            shape((1, hidden), F32),
            shape(terms.shape[1:], F32),
        ],
        in_specs=[vmem] * 8,
        out_specs=[vmem] * 8,
        scratch_shapes=[
            pltpu.VMEM((rows, hidden), BF),
            pltpu.VMEM((rows, hidden), BF),
            pltpu.VMEM((rows, width), BF),
            pltpu.VMEM((rows, width), F32),
            pltpu.VMEM((rows, 1), F32),
            pltpu.VMEM((rows, width), BF),
            pltpu.VMEM(terms.shape, BF),
        ]
        + reduce_scratch([terms], strips, depth),
        compiler_params=pltpu.CompilerParams(
            collective_id=collective_id, has_side_effects=True, vmem_limit_bytes=67043328
        ),
        name="middle",
    )(inputs, context, cotangent, w_out, w_up, w_down, plain, b_up.reshape(1, hidden))

EPS = 1e-06
AXES = ("fsdp", "rep")


def norm_forward(hidden, gain, shift):
    mean = jnp.mean(hidden, axis=-1, keepdims=True)
    centred = hidden - mean
    inverse = lax.rsqrt(jnp.mean(centred * centred, axis=-1, keepdims=True) + EPS)
    normed = centred * inverse
    return (normed * gain + shift, normed, inverse)


def norm_backward(grad_out, normed, inverse, gain):
    grad_normed = grad_out * gain
    grad_in = inverse * (
        grad_normed
        - jnp.mean(grad_normed, axis=-1, keepdims=True)
        - normed * jnp.mean(grad_normed * normed, axis=-1, keepdims=True)
    )
    return (grad_in, jnp.sum(grad_out * normed, axis=0), jnp.sum(grad_out, axis=0))


def column_sums(grad):
    return jnp.sum(grad.astype(F32), axis=0)


def gather_native(pieces):
    return [lax.all_gather(p, AXES, axis=0, tiled=False) for p in pieces]


def reduce_native(terms):
    return [lax.psum_scatter(t.astype(F32), AXES, scatter_dimension=0, tiled=False) for t in terms]


def local(
    mesh_shape,
    hidden_in,
    lengths,
    query_weight,
    key_weight,
    value_weight,
    out_weight,
    up_weight,
    down_weight,
    query_bias,
    value_bias,
    out_bias,
    up_bias,
    down_bias,
    first_gain,
    first_shift,
    second_gain,
    second_shift,
    cotangent,
):
    seqs, length, width = hidden_in.shape
    rows = seqs * length
    hidden = up_weight.shape[1]
    share = query_weight.shape[0]
    spread = hidden // width
    devices = width // share
    vectors = jnp.concatenate(
        [
            jnp.stack([query_bias, value_bias, out_bias, down_bias, first_gain, first_shift, second_gain, second_shift]),
            up_bias.reshape(spread, share),
        ]
    )
    count = vectors.shape[0]
    vector_slot = jnp.pad(vectors, ((0, -count % 16), (0, -share % 128)))
    qkv_shard = jnp.concatenate([query_weight, key_weight, value_weight], axis=1)
    later = [out_weight, up_weight, down_weight]
    fused = fits(mesh_shape, share)
    got = gather(mesh_shape, [vector_slot, qkv_shard])
    w_qkv = got[1].reshape(width, 3 * width)
    wide = got[0].astype(F32)
    plain = jnp.transpose(wide[:, :8, :share], (1, 0, 2)).reshape(8, width)
    b_query, b_values, b_out, b_down, gain_one, shift_one, gain_two, shift_two = [plain[i] for i in range(8)]
    b_up = wide[:, 8 : 8 + spread, :share].reshape(hidden)

    inputs = hidden_in.reshape(rows, width)
    b_qkv = jnp.concatenate([b_query, jnp.zeros_like(b_query), b_values])
    if fused:
        qkv, context, log_sums, got = forward_and_gather(mesh_shape, lengths, inputs, w_qkv, b_qkv, later)
    else:
        got = gather(mesh_shape, later)
        qkv = (nn(inputs, w_qkv) + b_qkv).astype(BF)
        context, log_sums = attention_forward(lengths, qkv, seqs, length, width)
    w_out = got[0].reshape(width, width)
    w_up = got[1].reshape(width, hidden)
    w_down = got[2].reshape(hidden, width)
    if fused:
        hidden_out, grad_first_sum, grad_context, grad_w_out, grad_w_up, vector_sums, grad_b_up, owned_down = middle(
            mesh_shape, inputs, context, cotangent.reshape(rows, width), w_out, w_up, w_down, plain, b_up
        )
        hidden_out = hidden_out.reshape(seqs, length, width)
        later = [grad_w_out.reshape(devices, share, width), grad_w_up.reshape(devices, share, hidden)]
        grad_w_qkv, input_grad, bias_sums, owned_later = backward_and_reduce(
            mesh_shape, lengths, inputs, w_qkv, qkv, grad_context, context, log_sums, grad_first_sum, later
        )
        owned_later = [owned_later[0], owned_later[1], owned_down]
        bias_sums = bias_sums[0]
        sums = jnp.concatenate([jnp.stack([bias_sums[:width], bias_sums[2 * width :]]), vector_sums[2:]])
    else:
        first_sum = inputs.astype(F32) + nn(context, w_out) + b_out
        first, normed_one, inverse_one = norm_forward(first_sum, gain_one, shift_one)
        first_low = first.astype(BF)
        inner = nn(first_low, w_up) + b_up
        half = 0.5 * (1.0 + lax.erf(inner * (2.0**-0.5)))
        active = (inner * half).astype(BF)
        slope = half + inner * ((2.0 * math.pi) ** -0.5) * jnp.exp(-0.5 * inner * inner)
        slope = slope.astype(BF)
        second_sum = first + nn(active, w_down) + b_down
        result, normed_two, inverse_two = norm_forward(second_sum, gain_two, shift_two)
        hidden_out = result.astype(BF).reshape(seqs, length, width)
        grad_out = cotangent.reshape(rows, width).astype(F32)
        grad_second, grad_gain_two, grad_shift_two = norm_backward(grad_out, normed_two, inverse_two, gain_two)
        grad_branch = grad_second.astype(BF)
        grad_b_down = column_sums(grad_branch)
        grad_w_down = tn(active, grad_branch)
        grad_active = nt(grad_branch, w_down)
        grad_inner = (grad_active * slope.astype(F32)).astype(BF)
        grad_b_up = column_sums(grad_inner)
        grad_w_up = tn(first_low, grad_inner)
        grad_first = grad_second + nt(grad_inner, w_up)
        grad_first_sum, grad_gain_one, grad_shift_one = norm_backward(grad_first, normed_one, inverse_one, gain_one)
        grad_attn = grad_first_sum.astype(BF)
        grad_b_out = column_sums(grad_attn)
        grad_w_out = tn(context, grad_attn)
        grad_context = nt(grad_attn, w_out).astype(BF)
        later = [
            grad_w_out.reshape(devices, share, width),
            grad_w_up.reshape(devices, share, hidden),
            grad_w_down.reshape(devices, spread * share, width),
        ]
        grad_query, grad_keys, grad_values = attention_backward(
            lengths, qkv, grad_context, context, log_sums, seqs, length, width
        )
        grad_qkv = jnp.concatenate([grad_query, grad_keys, grad_values], axis=1)
        input_grad = (grad_first_sum + nt(grad_qkv, w_qkv)).astype(BF)
        grad_w_qkv = tn(inputs, grad_qkv)
        bias_sums = column_sums(grad_qkv)
        owned_later = reduce_native(later)
        sums = jnp.stack(
            [
                bias_sums[:width],
                bias_sums[2 * width :],
                grad_b_out,
                grad_b_down,
                grad_gain_one,
                grad_shift_one,
                grad_gain_two,
                grad_shift_two,
            ]
        )
    input_grad = input_grad.reshape(seqs, length, width)
    vector_terms = jnp.concatenate(
        [jnp.transpose(sums.reshape(8, devices, share), (1, 0, 2)), grad_b_up.reshape(devices, spread, share)], axis=1
    )
    vector_terms = jnp.pad(vector_terms, ((0, 0), (0, -count % 16), (0, -share % 128)))
    owned = reduce(mesh_shape, [vector_terms, grad_w_qkv.reshape(devices, share, 3 * width)])
    vec = owned[0][:count, :share]
    return (
        hidden_out,
        input_grad,
        owned[1][:, :width],
        owned[1][:, width : 2 * width],
        owned[1][:, 2 * width :],
        owned_later[0],
        owned_later[1],
        owned_later[2],
        vec[0],
        vec[1],
        vec[2],
        vec[8:].reshape(spread * share),
        vec[3],
        vec[4],
        vec[5],
        vec[6],
        vec[7],
    )


def solution(mesh):
    rows = P(AXES, None)
    flat = P(AXES)
    cube = P(AXES, None, None)
    in_specs = (cube, flat) + (rows,) * 6 + (flat,) * 9 + (cube,)
    out_specs = (cube, cube) + (rows,) * 6 + (flat,) * 9
    body = functools.partial(local, dict(mesh.shape))
    return jax.shard_map(body, mesh=mesh, in_specs=in_specs, out_specs=out_specs, check_vma=False)
```

```python
import functools
import math

import jax
import jax.numpy as jnp
from jax import lax
from jax.experimental import pallas as pl
from jax.experimental.pallas import tpu as pltpu
from jax.sharding import PartitionSpec as P

HD = 64
PAIR = 2 * HD
BF = jnp.bfloat16
F32 = jnp.float32


def nt(left, right):
    return lax.dot_general(left, right, (((1,), (1,)), ((), ())), preferred_element_type=F32)


def nn(left, right):
    return jnp.dot(left, right, preferred_element_type=F32)


def tn(left, right):
    return lax.dot_general(left, right, (((0,), (0,)), ((), ())), preferred_element_type=F32)


def head_masks(length):
    lane = lax.broadcasted_iota(jnp.int32, (length, PAIR), 1)
    return lane


def masked_keys(k2, lane, head, valid):
    inside = (lane // HD) == head
    slot = lane == (1 - head) * HD
    row = lax.broadcasted_iota(jnp.int32, lane.shape, 0)
    bias = jnp.where(row < valid, 0.0, -1e30).astype(BF)
    return jnp.where(inside, k2, jnp.where(slot, bias, jnp.zeros_like(k2)))


def masked_query(q2, lane, head):
    inside = (lane // HD) == head
    slot = lane == (1 - head) * HD
    return jnp.where(inside, q2, jnp.where(slot, jnp.ones_like(q2), jnp.zeros_like(q2)))


def forward_pair(valid, q2, k2, v2):
    lane = head_masks(q2.shape[0])
    first = lane < HD
    q2 = q2 * BF(0.125)
    outs, tops = [], []
    for h in (0, 1):
        s = nt(masked_query(q2, lane, h), masked_keys(k2, lane, h, valid))
        top = jnp.max(s, axis=1, keepdims=True)
        e = jnp.exp(s - top).astype(BF)
        outs.append(nn(e, jnp.where((lane // HD) == h, v2, jnp.ones_like(v2))))
        tops.append(top)
    num = jnp.where(first, outs[0], outs[1])
    den = pltpu.roll(jnp.where(first, outs[1], outs[0]), HD, 1)
    lse = jnp.where(first, tops[0], tops[1]) + jnp.log(den)
    turned = lse.T
    return (num / den).astype(BF), turned[0:1], turned[HD : HD + 1]


def attention_forward_kernel(len_ref, q_ref, k_ref, v_ref, ctx_ref, lse_ref):
    ctx, low, high = forward_pair(len_ref[pl.program_id(0)], q_ref[...], k_ref[...], v_ref[...])
    ctx_ref[...] = ctx
    lse_ref[0, 0, 0:1, :] = low
    lse_ref[0, 0, 1:2, :] = high


def attention_forward(lengths, qkv, seqs, length, width):
    pairs = width // PAIR
    return pl.pallas_call(
        attention_forward_kernel,
        grid_spec=pltpu.PrefetchScalarGridSpec(
            num_scalar_prefetch=1,
            grid=(seqs, pairs),
            in_specs=[
                pl.BlockSpec((length, PAIR), lambda s, p, n: (s, p)),
                pl.BlockSpec((length, PAIR), lambda s, p, n: (s, pairs + p)),
                pl.BlockSpec((length, PAIR), lambda s, p, n: (s, 2 * pairs + p)),
            ],
            out_specs=[
                pl.BlockSpec((length, PAIR), lambda s, p, n: (s, p)),
                pl.BlockSpec((1, 1, 2, length), lambda s, p, n: (s, p, 0, 0)),
            ],
        ),
        out_shape=[
            jax.ShapeDtypeStruct((seqs * length, width), BF),
            jax.ShapeDtypeStruct((seqs, pairs, 2, length), F32),
        ],
        name="attention_forward",
    )(lengths, qkv, qkv, qkv)


def backward_pair(valid, q2, k2, v2, g2, ctx2, lses):
    lane = head_masks(q2.shape[0])
    first = lane < HD
    q2 = q2 * BF(0.125)
    k8 = k2 * BF(0.125)
    turned = (g2.astype(F32) * ctx2.astype(F32)).T
    dqs, dks, dvs = [], [], []
    for h in (0, 1):
        km = masked_keys(k2, lane, h, valid)
        qm = masked_query(q2, lane, h)
        vm = jnp.where((lane // HD) == h, v2, jnp.zeros_like(v2))
        delta = jnp.sum(turned[h * HD : (h + 1) * HD], axis=0, keepdims=True)
        p = jnp.exp(nt(km, qm) - lses[h])
        ds = (p * (nt(vm, g2) - delta)).astype(BF)
        dvs.append(nn(p.astype(BF), g2))
        dks.append(nn(ds, q2))
        dqs.append(tn(ds, k8))
    return [jnp.where(first, pair[0], pair[1]).astype(BF) for pair in (dqs, dks, dvs)]


def attention_backward_kernel(len_ref, q_ref, k_ref, v_ref, g_ref, ctx_ref, lse_ref, dq_ref, dk_ref, dv_ref):
    lses = [lse_ref[0, 0, h : h + 1, :] for h in (0, 1)]
    valid = len_ref[pl.program_id(0)]
    dq_ref[...], dk_ref[...], dv_ref[...] = backward_pair(
        valid, q_ref[...], k_ref[...], v_ref[...], g_ref[...], ctx_ref[...], lses
    )


def attention_backward(lengths, qkv, grad, ctx, lse, seqs, length, width):
    pairs = width // PAIR
    col = lambda k: pl.BlockSpec((length, PAIR), lambda s, p, n: (s, k * pairs + p))
    return pl.pallas_call(
        attention_backward_kernel,
        grid_spec=pltpu.PrefetchScalarGridSpec(
            num_scalar_prefetch=1,
            grid=(seqs, pairs),
            in_specs=[col(0), col(1), col(2), col(0), col(0), pl.BlockSpec((1, 1, 2, length), lambda s, p, n: (s, p, 0, 0))],
            out_specs=[col(0), col(0), col(0)],
        ),
        out_shape=[jax.ShapeDtypeStruct((seqs * length, width), BF)] * 3,
        name="attention_backward",
    )(lengths, qkv, qkv, qkv, grad, ctx, lse)


def neighbours():
    f, z = lax.axis_index("fsdp"), lax.axis_index("rep")
    core, x, y = f % 2, (f // 2) % 2, f // 4
    across_core = f + 1 - 2 * core
    step_x, step_y = 2 * (1 - 2 * x), 4 * (1 - 2 * y)
    return f, z, across_core, step_x, step_y


def remote(src, dst, send_sem, recv_sem, device):
    return pltpu.make_async_remote_copy(
        src_ref=src,
        dst_ref=dst,
        send_sem=send_sem,
        recv_sem=recv_sem,
        device_id=device,
        device_id_type=pl.DeviceIdType.MESH,
    )


def meet(depth, f, z, across_core, step_x, step_y):
    barrier = pltpu.get_barrier_semaphore()

    def greet(device):
        pl.semaphore_signal(barrier, inc=1, device_id=device, device_id_type=pl.DeviceIdType.MESH)

    for other in (across_core, f + step_x, f + step_y):
        greet((other, z))

    for hop in range(1, depth):
        greet((f, (z + hop) % depth))
    pl.semaphore_wait(barrier, 3 + depth - 1)


def far_first(step, z):
    zero = 3 * (1 - z // 2)
    one = (2 + 3 * z) % 5
    two = 1 + z % 2
    picks = (zero, one, two, z)
    total = 0
    for i, pick in enumerate(picks):
        hit = 1 - jnp.minimum(jnp.abs(step - i), 1)
        total = total + hit * pick
    return total


def strips_of(arrays):
    found = []
    for index, array in enumerate(arrays):
        columns = array[1]
        if columns % 256 == 0:
            found.append((index, 0, columns // 2, True))
            found.append((index, columns // 2, columns // 2, False))
        else:
            found.append((index, 0, None, True))
    return found


def cut(ref, strip):
    if strip[2] is None:
        return ref
    return ref.at[:, pl.ds(strip[1], strip[2])]


def gather_parts(depth, strips, ins, outs, sems):
    count = len(ins)
    (own_sem, up_sem, down_sem, first_sem, second_sem, relay_sem, core_sem) = sems[:7]
    (got_column, got_first, got_second, got_diagonal, got_core) = sems[7:]
    f, z, across_core, step_x, step_y = neighbours()

    def slot(who, plane):
        return who * depth + plane

    def place(n, who, plane):
        return cut(outs[strips[n][0]].at[slot(who, plane)], strips[n])

    def toward(n):
        return (step_x, step_y) if strips[n][3] else (step_y, step_x)

    def own_copy(a):
        return pltpu.make_async_copy(ins[a], outs[a].at[slot(f, z)], own_sem.at[a])

    def core_copy(n, kind, plane, src):
        first, second = toward(n)
        who = f + (0, first, second, first + second)[kind]
        where = place(n, who, plane)
        return remote(where if src is None else src, where, core_sem.at[n, kind, plane], got_core.at[n, kind, plane], (across_core, z))

    def core_arrival(n, kind, plane):
        first, second = toward(n)
        who = across_core + (0, first, second, first + second)[kind]
        where = place(n, who, plane)
        return remote(where, where, core_sem.at[n, kind, plane], got_core.at[n, kind, plane], (across_core, z))

    def column_up(n, plane, src):
        return remote(src, place(n, f, plane), up_sem.at[n, plane], got_column.at[n, plane], (f, z + 1))

    def column_down(n, plane, src):
        return remote(src, place(n, f, plane), down_sem.at[n, plane], got_column.at[n, plane], (f, z - 1))

    def to_first(n, plane, src):
        return remote(src, place(n, f, plane), first_sem.at[n, plane], got_first.at[n, plane], (f + toward(n)[0], z))

    def to_second(n, plane, src):
        return remote(src, place(n, f, plane), second_sem.at[n, plane], got_second.at[n, plane], (f + toward(n)[1], z))

    def relay(n, plane):
        where = place(n, f + toward(n)[0], plane)
        return remote(where, where, relay_sem.at[n, plane], got_diagonal.at[n, plane], (f + toward(n)[1], z))

    def each(body):
        for n in range(len(strips)):
            body(n)

    def send_own(n):
        src = cut(ins[strips[n][0]], strips[n])
        to_first(n, z, src).start()
        to_second(n, z, src).start()

        @pl.when(z < depth - 1)
        def _():
            column_up(n, z, src).start()

        @pl.when(z > 0)
        def _():
            column_down(n, z, src).start()

        core_copy(n, 0, z, src).start()

    def begin(greet=True):
        if greet:
            meet(depth, f, z, across_core, step_x, step_y)
        for a in range(count):
            own_copy(a).start()
        each(send_own)

    def phase(t):
        plane = far_first(depth - 1 - t, z)
        before = far_first(depth - t, z)
        earlier = far_first(depth + 1 - t, z)

        @pl.when((t >= 1) & (t < depth))
        def _():
            def arrived(n):
                src = place(n, f, plane)
                remote(src, src, up_sem.at[n, plane], got_column.at[n, plane], (f, z)).wait_recv()
                to_first(n, plane, src).start()
                to_second(n, plane, src).start()

                @pl.when((plane < z) & (z < depth - 1))
                def _():
                    column_up(n, plane, src).start()

                @pl.when((plane > z) & (z > 0))
                def _():
                    column_down(n, plane, src).start()

                core_copy(n, 0, plane, None).start()

            each(arrived)

        @pl.when((t >= 1) & (t < depth + 1))
        def _():
            def beside(n):
                first, second = toward(n)
                here = place(n, f + first, before)
                remote(here, here, first_sem.at[n, before], got_first.at[n, before], (f + first, z)).wait_recv()
                relay(n, before).start()
                core_copy(n, 1, before, None).start()

            each(beside)

            def above(n):
                first, second = toward(n)
                here = place(n, f + second, before)
                remote(here, here, second_sem.at[n, before], got_second.at[n, before], (f + second, z)).wait_recv()
                core_copy(n, 2, before, None).start()

            each(above)

        @pl.when(t >= 2)
        def _():
            def opposite(n):
                first, second = toward(n)
                here = place(n, f + first + second, earlier)
                remote(here, here, relay_sem.at[n, earlier], got_diagonal.at[n, earlier], (f + second, z)).wait_recv()
                core_copy(n, 3, earlier, None).start()

            each(opposite)

    def close_plane(plane, carry):
        def close(n):
            src = place(n, f, plane)
            to_first(n, plane, src).wait_send()
            to_second(n, plane, src).wait_send()
            relay(n, plane).wait_send()

            @pl.when((plane <= z) & (z < depth - 1))
            def _():
                column_up(n, plane, src).wait_send()

            @pl.when((plane >= z) & (z > 0))
            def _():
                column_down(n, plane, src).wait_send()

            for kind in range(4):
                core_copy(n, kind, plane, None).wait_send()
                core_arrival(n, kind, plane).wait_recv()

        each(close)
        return carry

    def finish():
        for a in range(count):
            own_copy(a).wait()
        lax.fori_loop(0, depth, close_plane, 0)

    return begin, phase, finish


def gather_semaphores(strips, count, depth):
    dma = pltpu.SemaphoreType.DMA
    flat, cored = dma((len(strips), depth)), dma((len(strips), 4, depth))
    return [dma((count,)), flat, flat, flat, flat, flat, cored, flat, flat, flat, flat, cored]


def fits(mesh_shape, share):
    return mesh_shape["fsdp"] == 8 and mesh_shape["rep"] == 4 and share % 8 == 0


def reduce_parts(depth, strips, terms, outs, scratch):
    count = len(terms)
    mine, theirs, relayed, direct, partial, below, above = (scratch[i * count : (i + 1) * count] for i in range(7))
    sems = scratch[7 * count :]
    (own_sem, core_sem, relay_sem, direct_sem, partial_sem, up_sem, down_sem) = sems[:7]
    (got_core, got_relay, got_direct, got_partial, got_below, got_above) = sems[7:]
    f, z, across_core, step_x, step_y = neighbours()

    def toward(n):
        return (step_x, step_y) if strips[n][3] else (step_y, step_x)

    def steps(n):
        first, second = toward(n)
        return (0, first, second, first + second)

    def term(n, who, plane):
        return cut(terms[strips[n][0]].at[who * depth + plane], strips[n])

    def cell(family, n, *index):
        return cut(family[strips[n][0]].at[index], strips[n])

    def own_copy(n, kind, plane):
        return pltpu.make_async_copy(term(n, f + steps(n)[kind], plane), cell(mine, n, kind, plane), own_sem.at[n, kind, plane])

    def core_copy(n, kind, plane):
        return remote(
            term(n, across_core + steps(n)[kind], plane),
            cell(theirs, n, kind, plane),
            core_sem.at[n, kind, plane],
            got_core.at[n, kind, plane],
            (across_core, z),
        )

    def relay(n, plane):
        return remote(cell(theirs, n, 3, plane), cell(relayed, n, plane), relay_sem.at[n, plane], got_relay.at[n, plane], (f + toward(n)[1], z))

    def straight(n, plane):
        return remote(cell(theirs, n, 2, plane), cell(direct, n, plane), direct_sem.at[n, plane], got_direct.at[n, plane], (f + toward(n)[1], z))

    def second_hop(n, plane):
        return remote(cell(theirs, n, 1, plane), cell(partial, n, plane), partial_sem.at[n, plane], got_partial.at[n, plane], (f + toward(n)[0], z))

    def go_up(n, plane):
        return remote(cell(theirs, n, 0, plane), cell(below, n, plane), up_sem.at[n, plane], got_below.at[n, plane], (f, z + 1))

    def go_down(n, plane):
        return remote(cell(theirs, n, 0, plane), cell(above, n, plane), down_sem.at[n, plane], got_above.at[n, plane], (f, z - 1))

    def add(n, kind, plane, *others):
        here = cell(theirs, n, kind, plane)
        total = here[...].astype(F32)
        for other in others:
            total = total + other[...].astype(F32)
        here[...] = total.astype(here.dtype)

    each = range(len(strips))
    order = (3, 2, 1, 0)

    def launch(t, carry):
        plane = far_first(t, z)
        for kind in order:
            for n in each:
                core_copy(n, kind, plane).start()
                own_copy(n, kind, plane).start()
        return carry

    def begin(greet=True):
        if greet:
            meet(depth, f, z, across_core, step_x, step_y)
        lax.fori_loop(0, depth, launch, 0)

    def phase(t):
        plane = far_first(t, z)
        before = far_first(t - 1, z)
        earlier = far_first(t - 2, z)

        @pl.when(t < depth)
        def _():
            for kind in order:
                for n in each:
                    core_copy(n, kind, plane).wait_recv()
                    own_copy(n, kind, plane).wait()
                    add(n, kind, plane, cell(mine, n, kind, plane))
                if kind == 3:
                    for n in each:
                        relay(n, plane).start()
                if kind == 2:
                    for n in each:
                        straight(n, plane).start()

        @pl.when((t >= 1) & (t < depth + 1))
        def _():
            for n in each:
                relay(n, before).wait_recv()
                add(n, 1, before, cell(relayed, n, before))
            for n in each:
                second_hop(n, before).start()

        @pl.when(t >= 2)
        def _():
            for n in each:
                straight(n, earlier).wait_recv()
                second_hop(n, earlier).wait_recv()
                add(n, 0, earlier, cell(direct, n, earlier), cell(partial, n, earlier))

            @pl.when((earlier >= z) & (z > 0))
            def _():
                for n in each:
                    go_up(n, earlier).wait_recv()
                    add(n, 0, earlier, cell(below, n, earlier))

            @pl.when((earlier <= z) & (z < depth - 1))
            def _():
                for n in each:
                    go_down(n, earlier).wait_recv()
                    add(n, 0, earlier, cell(above, n, earlier))

            @pl.when(earlier > z)
            def _():
                for n in each:
                    go_up(n, earlier).start()

            @pl.when(earlier < z)
            def _():
                for n in each:
                    go_down(n, earlier).start()

    def close_plane(plane, carry):
        for n in each:
            for kind in order:
                core_copy(n, kind, plane).wait_send()
            relay(n, plane).wait_send()
            straight(n, plane).wait_send()
            second_hop(n, plane).wait_send()

        @pl.when(plane > z)
        def _():
            for n in each:
                go_up(n, plane).wait_send()

        @pl.when(plane < z)
        def _():
            for n in each:
                go_down(n, plane).wait_send()

        return carry

    def finish():
        for a in range(count):
            outs[a][...] = theirs[a][0, z].astype(F32)
        lax.fori_loop(0, depth, close_plane, 0)

    return begin, phase, finish


def reduce_scratch(terms, strips, depth):
    dma = pltpu.SemaphoreType.DMA
    flat, cored = dma((len(strips), depth)), dma((len(strips), 4, depth))
    whole = [pltpu.VMEM((4, depth) + t.shape[1:], t.dtype) for t in terms]
    line = [pltpu.VMEM((depth,) + t.shape[1:], t.dtype) for t in terms]
    return whole + whole + line * 5 + [cored, cored, flat, flat, flat, flat, flat, cored, flat, flat, flat, flat, flat]


def lane_block(index, size):
    return pl.ds(pl.multiple_of(index * size, size), size)


def forward_kernel(depth, strips, counts, len_ref, x_ref, *refs):
    early, later = counts
    ins, refs = refs[: early + later], refs[early + later :]
    qkv_ref, ctx_ref, lse_ref, vec_ref = refs[:4]
    outs, sems = refs[4 : 4 + early + later], refs[4 + early + later :]
    kinds = len(sems) // 2
    first = gather_parts(depth, strips[0], ins[:early], outs[:early], sems[:kinds])
    second = gather_parts(depth, strips[1], ins[early:], outs[early:], sems[kinds:])
    slots_ref, w_ref = outs[:early]
    rows, width = x_ref.shape
    seqs = len_ref.shape[0]
    length = rows // seqs
    block = 2 * PAIR

    first[0]()
    second[0](greet=False)

    def arrive(t, carry):
        first[1](t)

        @pl.when((t >= depth - 1) & (t <= depth))
        def _():
            second[1](t - depth + 2)

        return carry

    lax.fori_loop(1, depth + 2, arrive, 0)
    first[2]()
    vec_ref[...] = jnp.sum(slots_ref[...].astype(F32), axis=0)

    def step(t, carry):
        j = t // 2

        @pl.when(t % 2 == 0)
        def _():
            for part in range(3):
                columns = pl.ds(pl.multiple_of(part * width + j * block, block), block)
                made = nn(x_ref[...], w_ref[:, :, columns].reshape(width, block))
                if part != 1:
                    made = made + vec_ref[part // 2 : part // 2 + 1, lane_block(j, block)]
                qkv_ref[:, columns] = made.astype(BF)

        @pl.when(t % 2 == 1)
        def _():
            def attend(i, inner):
                s, p = i // 2, j * 2 + i % 2
                part_rows = lane_block(s, length)
                q2, k2, v2 = (
                    qkv_ref[part_rows, pl.ds(pl.multiple_of(part * width + p * PAIR, PAIR), PAIR)] for part in range(3)
                )
                ctx, low, high = forward_pair(len_ref[s], q2, k2, v2)
                ctx_ref[part_rows, lane_block(p, PAIR)] = ctx
                lse_ref[s, p, 0:1, :] = low
                lse_ref[s, p, 1:2, :] = high
                return inner

            lax.fori_loop(0, seqs * 2, attend, 0)

        @pl.when(t % 2 == 0)
        def _():
            second[1](depth - 1 + j)

        return carry

    lax.fori_loop(0, depth + 2, step, 0)
    second[2]()


def forward_and_gather(mesh_shape, lengths, inputs, early, later, collective_id=3):
    depth, devices = mesh_shape["rep"], mesh_shape["rep"] * mesh_shape["fsdp"]
    strips = [strips_of([p.shape for p in group]) for group in (early, later)]
    counts = (len(early), len(later))
    rows, width = inputs.shape
    seqs = lengths.shape[0]
    pairs = width // PAIR
    vmem, away = pl.BlockSpec(memory_space=pltpu.VMEM), pl.BlockSpec(memory_space=pl.ANY)
    out = pl.pallas_call(
        functools.partial(forward_kernel, depth, strips, counts),
        out_shape=[
            jax.ShapeDtypeStruct((rows, 3 * width), BF),
            jax.ShapeDtypeStruct((rows, width), BF),
            jax.ShapeDtypeStruct((seqs, pairs, 2, rows // seqs), F32),
            jax.ShapeDtypeStruct(early[0].shape, F32),
        ]
        + [jax.ShapeDtypeStruct((devices,) + p.shape, p.dtype) for p in early + later],
        in_specs=[pl.BlockSpec(memory_space=pltpu.SMEM)] + [vmem] * (1 + sum(counts)),
        out_specs=[vmem] * (4 + counts[0]) + [away] * counts[1],
        scratch_shapes=gather_semaphores(strips[0], counts[0], depth) + gather_semaphores(strips[1], counts[1], depth),
        compiler_params=pltpu.CompilerParams(
            collective_id=collective_id, has_side_effects=True, vmem_limit_bytes=48 * 1024 * 1024
        ),
        name="forward_and_gather",
    )(lengths, inputs, *early, *later)
    return out[0], out[1], out[2], out[3], out[5], out[6:]


def reduce_kernel(depth, strips, count, *refs):
    terms, outs, scratch = refs[:count], refs[count : 2 * count], refs[2 * count :]
    begin, phase, finish = reduce_parts(depth, strips, terms, outs, scratch)
    begin()

    def step(t, carry):
        phase(t)
        return carry

    lax.fori_loop(0, depth + 2, step, 0)
    finish()


def reduce_remote(mesh_shape, terms, collective_id=2):
    depth = mesh_shape["rep"]
    strips = strips_of([t.shape[1:] for t in terms])
    count = len(terms)
    return pl.pallas_call(
        functools.partial(reduce_kernel, depth, strips, count),
        out_shape=[jax.ShapeDtypeStruct(t.shape[1:], F32) for t in terms],
        in_specs=[pl.BlockSpec(memory_space=pl.ANY)] * count,
        out_specs=[pl.BlockSpec(memory_space=pltpu.VMEM)] * count,
        scratch_shapes=reduce_scratch(terms, strips, depth),
        compiler_params=pltpu.CompilerParams(
            collective_id=collective_id, has_side_effects=True, vmem_limit_bytes=48 * 1024 * 1024
        ),
        name="reduce_terms",
    )(*terms)


def backward_kernel(depth, strips, count, heads_at_once, len_ref, x_ref, w_ref, qkv_ref, g_ref, ctx_ref, lse_ref, sum_ref, *refs):
    terms, refs = refs[:count], refs[count:]
    dw_ref, dx_ref, bias_ref = refs[:3]
    outs, refs = refs[3 : 3 + count], refs[3 + count :]
    dqkv_ref, total_ref, scratch = refs[0], refs[1], refs[2:]
    begin, phase, finish = reduce_parts(depth, strips, terms, outs, scratch)
    width = x_ref.shape[1]
    seqs = len_ref.shape[0]
    length = x_ref.shape[0] // seqs
    block = heads_at_once * PAIR
    begin()
    total_ref[...] = sum_ref[...]

    def step(t, carry):
        j = t // 2

        @pl.when(t % 2 == 0)
        def _():
            def attend(i, inner):
                s, p = i // heads_at_once, j * heads_at_once + i % heads_at_once
                rows = lane_block(s, length)
                places = [pl.ds(pl.multiple_of(part * width + p * PAIR, PAIR), PAIR) for part in range(3)]
                own = lane_block(p, PAIR)
                q2, k2, v2 = (qkv_ref[rows, place] for place in places)
                lses = [lse_ref[s, p, h : h + 1, :] for h in (0, 1)]
                grads = backward_pair(len_ref[s], q2, k2, v2, g_ref[rows, own], ctx_ref[rows, own], lses)
                for place, grad in zip(places, grads):
                    dqkv_ref[rows, place] = grad
                return inner

            lax.fori_loop(0, seqs * heads_at_once, attend, 0)

        @pl.when(t % 2 == 1)
        def _():
            for part in range(3):
                columns = pl.ds(pl.multiple_of(part * width + j * block, block), block)
                grad = dqkv_ref[:, columns]
                dw_ref[:, columns] = tn(x_ref[...], grad).astype(BF)
                bias_ref[:, columns] = jnp.sum(grad.astype(F32), axis=0, keepdims=True)
                total_ref[...] += nt(grad, w_ref[:, columns])

        phase(t)
        return carry

    lax.fori_loop(0, depth + 2, step, 0)
    dx_ref[...] = total_ref[...].astype(BF)
    finish()


def backward_and_reduce(mesh_shape, lengths, inputs, w_qkv, qkv, grad, ctx, lse, grad_sum, terms, collective_id=4):
    depth = mesh_shape["rep"]
    strips = strips_of([t.shape[1:] for t in terms])
    count = len(terms)
    rows, width = inputs.shape
    pairs = width // PAIR
    vmem = pl.BlockSpec(memory_space=pltpu.VMEM)
    out = pl.pallas_call(
        functools.partial(backward_kernel, depth, strips, count, pairs * 2 // (depth + 2)),
        out_shape=[
            jax.ShapeDtypeStruct((width, 3 * width), BF),
            jax.ShapeDtypeStruct((rows, width), BF),
            jax.ShapeDtypeStruct((1, 3 * width), F32),
        ]
        + [jax.ShapeDtypeStruct(t.shape[1:], F32) for t in terms],
        in_specs=[pl.BlockSpec(memory_space=pltpu.SMEM)] + [vmem] * 7 + [pl.BlockSpec(memory_space=pl.ANY)] * count,
        out_specs=[vmem] * (3 + count),
        scratch_shapes=[pltpu.VMEM((rows, 3 * width), BF), pltpu.VMEM((rows, width), F32)] + reduce_scratch(terms, strips, depth),
        compiler_params=pltpu.CompilerParams(
            collective_id=collective_id, has_side_effects=True, vmem_limit_bytes=63 * 1024 * 1024
        ),
        name="backward_and_reduce",
    )(lengths, inputs, w_qkv, qkv, grad, ctx, lse, grad_sum, *terms)
    return out[0], out[1], out[2], out[3:]


def norm_stats(hidden):
    mean = jnp.mean(hidden, axis=-1, keepdims=True)
    centred = hidden - mean
    inverse = lax.rsqrt(jnp.mean(centred * centred, axis=-1, keepdims=True) + EPS)
    return centred * inverse, inverse


def norm_pull(grad_normed, normed, inverse):
    return inverse * (
        grad_normed
        - jnp.mean(grad_normed, axis=-1, keepdims=True)
        - normed * jnp.mean(grad_normed * normed, axis=-1, keepdims=True)
    )


def total_rows(value):
    return jnp.sum(value.astype(F32), axis=0, keepdims=True)


def middle_kernel(depth, strips, x_ref, ctx_ref, cot_ref, w_out_ref, w_up_ref, w_down_ref, vec_ref, *refs):
    hidden_ref, sum_ref, grad_ctx_ref, dw_out_ref, dw_up_ref, vec_out_ref, owned_ref = refs[:7]
    active_ref, slope_ref, low_ref, normed_ref, inverse_ref, branch_ref, terms_ref = refs[7:14]
    begin, phase, finish = reduce_parts(depth, strips, (terms_ref,), (owned_ref,), refs[14:])
    rows, width = x_ref.shape
    hidden = w_up_ref.shape[1]
    chunk, block = 256, 256

    def vector(i):
        return vec_ref[i : i + 1, :]

    def up_place(j):
        return pl.ds(8 + j // (width // block), 1), lane_block(j % (width // block), block)

    def put(i, value):
        vec_out_ref[i : i + 1, :] += value

    vec_out_ref[...] = jnp.zeros_like(vec_out_ref)

    def attention_out(i, carry):
        part = lane_block(i, chunk)
        first_sum = x_ref[part, :].astype(F32) + nn(ctx_ref[part, :], w_out_ref[...]) + vector(2)
        normed, inverse = norm_stats(first_sum)
        first = normed * vector(4) + vector(5)
        normed_ref[part, :] = normed
        inverse_ref[part, :] = inverse
        sum_ref[part, :] = first
        low_ref[part, :] = first.astype(BF)
        return carry

    lax.fori_loop(0, rows // chunk, attention_out, 0)

    def up(j, carry):
        columns = lane_block(j, block)
        inner = nn(low_ref[...], w_up_ref[:, columns]) + vec_ref[up_place(j)]
        half = 0.5 + 0.5 * lax.erf(inner * (2.0**-0.5))
        active_ref[:, columns] = (inner * half).astype(BF)
        slope_ref[:, columns] = (half + inner * ((2.0 * math.pi) ** -0.5) * jnp.exp(-0.5 * inner * inner)).astype(BF)
        return carry

    lax.fori_loop(0, hidden // block, up, 0)

    def down(i, carry):
        part = lane_block(i, chunk)
        second_sum = sum_ref[part, :] + nn(active_ref[part, :], w_down_ref[...]) + vector(3)
        normed, inverse = norm_stats(second_sum)
        hidden_ref[part, :] = (normed * vector(6) + vector(7)).astype(BF)
        grad_out = cot_ref[part, :].astype(F32)
        put(6, total_rows(grad_out * normed))
        put(7, total_rows(grad_out))
        grad_second = norm_pull(grad_out * vector(6), normed, inverse)
        sum_ref[part, :] = grad_second
        branch = grad_second.astype(BF)
        branch_ref[part, :] = branch
        put(3, total_rows(branch))
        return carry

    lax.fori_loop(0, rows // chunk, down, 0)

    share = terms_ref.shape[1]
    slots = 4

    def down_terms(i, carry):
        term = tn(active_ref[:, lane_block(i, slots * share)], branch_ref[...])
        terms_ref[pl.ds(i * slots, slots)] = term.astype(BF).reshape(slots, share, width)
        return carry

    lax.fori_loop(0, terms_ref.shape[0] // slots, down_terms, 0)
    begin()
    blocks = hidden // block
    stride = blocks // depth

    def up_back(j, carry):
        columns = lane_block(j, block)
        grad_active = nt(branch_ref[...], w_down_ref[columns, :])
        grad_inner = (grad_active * slope_ref[:, columns].astype(F32)).astype(BF)
        slope_ref[:, columns] = grad_inner
        vec_out_ref[up_place(j)] = total_rows(grad_inner)
        dw_up_ref[:, columns] = tn(low_ref[...], grad_inner).astype(BF)

        @pl.when(j % stride == stride - 1)
        def _():
            phase(j // stride)

        return carry

    lax.fori_loop(0, blocks, up_back, 0)

    def first_back(i, carry):
        part = lane_block(i, chunk)
        grad_first = sum_ref[part, :] + nt(slope_ref[part, :], w_up_ref[...])
        normed = normed_ref[part, :]
        put(4, total_rows(grad_first * normed))
        put(5, total_rows(grad_first))
        grad = norm_pull(grad_first * vector(4), normed, inverse_ref[part, :])
        sum_ref[part, :] = grad
        low = grad.astype(BF)
        branch_ref[part, :] = low
        put(2, total_rows(low))
        grad_ctx_ref[part, :] = nt(low, w_out_ref[...]).astype(BF)
        return carry

    lax.fori_loop(0, rows // chunk, first_back, 0)
    dw_out_ref[...] = tn(ctx_ref[...], branch_ref[...]).astype(BF)
    lax.fori_loop(depth, depth + 2, lambda t, carry: (phase(t), carry)[1], 0)
    finish()


def middle(mesh_shape, inputs, context, cotangent, w_out, w_up, w_down, vectors, collective_id=5):
    depth, devices = mesh_shape["rep"], mesh_shape["rep"] * mesh_shape["fsdp"]
    rows, width = inputs.shape
    hidden = w_up.shape[1]
    terms = jax.ShapeDtypeStruct((devices, hidden // devices, width), BF)
    strips = strips_of([terms.shape[1:]])
    vmem = pl.BlockSpec(memory_space=pltpu.VMEM)
    shape = jax.ShapeDtypeStruct
    return pl.pallas_call(
        functools.partial(middle_kernel, depth, strips),
        out_shape=[
            shape((rows, width), BF),
            shape((rows, width), F32),
            shape((rows, width), BF),
            shape((width, width), BF),
            shape((width, hidden), BF),
            shape(vectors.shape, F32),
            shape(terms.shape[1:], F32),
        ],
        in_specs=[vmem] * 7,
        out_specs=[vmem] * 7,
        scratch_shapes=[
            pltpu.VMEM((rows, hidden), BF),
            pltpu.VMEM((rows, hidden), BF),
            pltpu.VMEM((rows, width), BF),
            pltpu.VMEM((rows, width), F32),
            pltpu.VMEM((rows, 1), F32),
            pltpu.VMEM((rows, width), BF),
            pltpu.VMEM(terms.shape, BF),
        ]
        + reduce_scratch([terms], strips, depth),
        compiler_params=pltpu.CompilerParams(
            collective_id=collective_id, has_side_effects=True, vmem_limit_bytes=67043328
        ),
        name="middle",
    )(inputs, context, cotangent, w_out, w_up, w_down, vectors)

EPS = 1e-06
AXES = ("fsdp", "rep")


def norm_forward(hidden, gain, shift):
    mean = jnp.mean(hidden, axis=-1, keepdims=True)
    centred = hidden - mean
    inverse = lax.rsqrt(jnp.mean(centred * centred, axis=-1, keepdims=True) + EPS)
    normed = centred * inverse
    return (normed * gain + shift, normed, inverse)


def norm_backward(grad_out, normed, inverse, gain):
    grad_normed = grad_out * gain
    grad_in = inverse * (
        grad_normed
        - jnp.mean(grad_normed, axis=-1, keepdims=True)
        - normed * jnp.mean(grad_normed * normed, axis=-1, keepdims=True)
    )
    return (grad_in, jnp.sum(grad_out * normed, axis=0), jnp.sum(grad_out, axis=0))


def column_sums(grad):
    return jnp.sum(grad.astype(F32), axis=0)


def gather_native(pieces):
    return [lax.all_gather(p, AXES, axis=0, tiled=False) for p in pieces]


def reduce_native(terms):
    return [lax.psum_scatter(t.astype(F32), AXES, scatter_dimension=0, tiled=False) for t in terms]


def local_fused(mesh_shape, hidden_in, lengths, qkv_shard, later, vectors, up_bias, cotangent):
    seqs, length, width = hidden_in.shape
    rows = seqs * length
    depth = mesh_shape["rep"]
    devices = depth * mesh_shape["fsdp"]
    share, spread = width // devices, up_bias.shape[0] * devices // width
    hidden = width * spread
    me = lax.axis_index("fsdp") * depth + lax.axis_index("rep")
    column = lax.broadcasted_iota(jnp.int32, (8, width), 1)
    plain = jnp.where(column // share == me, jnp.tile(jnp.stack(vectors), (1, devices)), 0)
    column = lax.broadcasted_iota(jnp.int32, (spread, width), 1) + width * lax.broadcasted_iota(jnp.int32, (spread, width), 0)
    wide = jnp.where(column // (spread * share) == me, jnp.tile(up_bias, (spread, devices // spread)), 0)
    slot = jnp.pad(jnp.concatenate([plain, wide]), ((0, -(8 + spread) % 16), (0, 0)))
    inputs = hidden_in.reshape(rows, width)
    qkv, context, log_sums, whole, w_qkv, got = forward_and_gather(mesh_shape, lengths, inputs, [slot, qkv_shard], later)
    w_qkv = w_qkv.reshape(width, 3 * width)
    w_out = got[0].reshape(width, width)
    w_up = got[1].reshape(width, hidden)
    w_down = got[2].reshape(hidden, width)
    hidden_out, grad_first_sum, grad_context, grad_w_out, grad_w_up, sums, owned_down = middle(
        mesh_shape, inputs, context, cotangent.reshape(rows, width), w_out, w_up, w_down, whole
    )
    terms = [grad_w_out.reshape(devices, share, width), grad_w_up.reshape(devices, share, hidden)]
    grad_w_qkv, input_grad, bias_sums, owned = backward_and_reduce(
        mesh_shape, lengths, inputs, w_qkv, qkv, grad_context, context, log_sums, grad_first_sum, terms
    )
    bias_sums = bias_sums.reshape(3, width)
    plain = jnp.concatenate([bias_sums[:1], bias_sums[2:], sums[2:8]]).reshape(8, devices, share)
    wide = sums[8 : 8 + spread].reshape(devices, spread, share)
    vector_terms = jnp.concatenate([jnp.transpose(plain, (1, 0, 2)), wide], axis=1)
    vector_terms = jnp.pad(vector_terms, ((0, 0), (0, -(8 + spread) % 16), (0, -share % 128)))
    summed, owned_qkv = reduce_remote(mesh_shape, [vector_terms, grad_w_qkv.reshape(devices, share, 3 * width)])
    vec = summed[:8, :share]
    up = summed[8 : 8 + spread, :share].reshape(spread * share)
    owned_qkv = [owned_qkv[:, part * width : (part + 1) * width] for part in range(3)]
    return (
        hidden_out.reshape(seqs, length, width),
        input_grad.reshape(seqs, length, width),
        *owned_qkv,
        *owned,
        owned_down,
        vec[0],
        vec[1],
        vec[2],
        up,
        *(vec[i] for i in range(3, 8)),
    )


def local(
    mesh_shape,
    hidden_in,
    lengths,
    query_weight,
    key_weight,
    value_weight,
    out_weight,
    up_weight,
    down_weight,
    query_bias,
    value_bias,
    out_bias,
    up_bias,
    down_bias,
    first_gain,
    first_shift,
    second_gain,
    second_shift,
    cotangent,
):
    if fits(mesh_shape, query_weight.shape[0]):
        return local_fused(
            mesh_shape,
            hidden_in,
            lengths,
            jnp.concatenate([query_weight, key_weight, value_weight], axis=1),
            [out_weight, up_weight, down_weight],
            [query_bias, value_bias, out_bias, down_bias, first_gain, first_shift, second_gain, second_shift],
            up_bias,
            cotangent,
        )
    seqs, length, width = hidden_in.shape
    rows = seqs * length
    hidden = up_weight.shape[1]
    share = query_weight.shape[0]
    spread = hidden // width
    devices = width // share
    vectors = jnp.concatenate(
        [
            jnp.stack([query_bias, value_bias, out_bias, down_bias, first_gain, first_shift, second_gain, second_shift]),
            up_bias.reshape(spread, share),
        ]
    )
    count = vectors.shape[0]
    vector_slot = jnp.pad(vectors, ((0, -count % 16), (0, -share % 128)))
    qkv_shard = jnp.concatenate([query_weight, key_weight, value_weight], axis=1)
    later = [out_weight, up_weight, down_weight]
    got = gather_native([vector_slot, qkv_shard])
    w_qkv = got[1].reshape(width, 3 * width)
    wide = got[0].astype(F32)
    plain = jnp.transpose(wide[:, :8, :share], (1, 0, 2)).reshape(8, width)
    b_query, b_values, b_out, b_down, gain_one, shift_one, gain_two, shift_two = [plain[i] for i in range(8)]
    b_up = wide[:, 8 : 8 + spread, :share].reshape(hidden)

    inputs = hidden_in.reshape(rows, width)
    b_qkv = jnp.concatenate([b_query, jnp.zeros_like(b_query), b_values])
    got = gather_native(later)
    qkv = (nn(inputs, w_qkv) + b_qkv).astype(BF)
    context, log_sums = attention_forward(lengths, qkv, seqs, length, width)
    w_out = got[0].reshape(width, width)
    w_up = got[1].reshape(width, hidden)
    w_down = got[2].reshape(hidden, width)
    first_sum = inputs.astype(F32) + nn(context, w_out) + b_out
    first, normed_one, inverse_one = norm_forward(first_sum, gain_one, shift_one)
    first_low = first.astype(BF)
    inner = nn(first_low, w_up) + b_up
    half = 0.5 * (1.0 + lax.erf(inner * (2.0**-0.5)))
    active = (inner * half).astype(BF)
    slope = half + inner * ((2.0 * math.pi) ** -0.5) * jnp.exp(-0.5 * inner * inner)
    slope = slope.astype(BF)
    second_sum = first + nn(active, w_down) + b_down
    result, normed_two, inverse_two = norm_forward(second_sum, gain_two, shift_two)
    hidden_out = result.astype(BF).reshape(seqs, length, width)
    grad_out = cotangent.reshape(rows, width).astype(F32)
    grad_second, grad_gain_two, grad_shift_two = norm_backward(grad_out, normed_two, inverse_two, gain_two)
    grad_branch = grad_second.astype(BF)
    grad_b_down = column_sums(grad_branch)
    grad_w_down = tn(active, grad_branch)
    grad_active = nt(grad_branch, w_down)
    grad_inner = (grad_active * slope.astype(F32)).astype(BF)
    grad_b_up = column_sums(grad_inner)
    grad_w_up = tn(first_low, grad_inner)
    grad_first = grad_second + nt(grad_inner, w_up)
    grad_first_sum, grad_gain_one, grad_shift_one = norm_backward(grad_first, normed_one, inverse_one, gain_one)
    grad_attn = grad_first_sum.astype(BF)
    grad_b_out = column_sums(grad_attn)
    grad_w_out = tn(context, grad_attn)
    grad_context = nt(grad_attn, w_out).astype(BF)
    later = [
        grad_w_out.reshape(devices, share, width),
        grad_w_up.reshape(devices, share, hidden),
        grad_w_down.reshape(devices, spread * share, width),
    ]
    grad_query, grad_keys, grad_values = attention_backward(
        lengths, qkv, grad_context, context, log_sums, seqs, length, width
    )
    grad_qkv = jnp.concatenate([grad_query, grad_keys, grad_values], axis=1)
    input_grad = (grad_first_sum + nt(grad_qkv, w_qkv)).astype(BF)
    grad_w_qkv = tn(inputs, grad_qkv)
    bias_sums = column_sums(grad_qkv)
    owned_later = reduce_native(later)
    sums = jnp.stack(
        [
            bias_sums[:width],
            bias_sums[2 * width :],
            grad_b_out,
            grad_b_down,
            grad_gain_one,
            grad_shift_one,
            grad_gain_two,
            grad_shift_two,
        ]
    )
    input_grad = input_grad.reshape(seqs, length, width)
    vector_terms = jnp.concatenate(
        [jnp.transpose(sums.reshape(8, devices, share), (1, 0, 2)), grad_b_up.reshape(devices, spread, share)], axis=1
    )
    vector_terms = jnp.pad(vector_terms, ((0, 0), (0, -count % 16), (0, -share % 128)))
    owned = reduce_native([vector_terms, grad_w_qkv.reshape(devices, share, 3 * width)])
    vec = owned[0][:count, :share]
    return (
        hidden_out,
        input_grad,
        owned[1][:, :width],
        owned[1][:, width : 2 * width],
        owned[1][:, 2 * width :],
        owned_later[0],
        owned_later[1],
        owned_later[2],
        vec[0],
        vec[1],
        vec[2],
        vec[8:].reshape(spread * share),
        vec[3],
        vec[4],
        vec[5],
        vec[6],
        vec[7],
    )


def solution(mesh):
    rows = P(AXES, None)
    flat = P(AXES)
    cube = P(AXES, None, None)
    in_specs = (cube, flat) + (rows,) * 6 + (flat,) * 9 + (cube,)
    out_specs = (cube, cube) + (rows,) * 6 + (flat,) * 9
    body = functools.partial(local, dict(mesh.shape))
    return jax.shard_map(body, mesh=mesh, in_specs=in_specs, out_specs=out_specs, check_vma=False)
```
